128 devices in a mesh: px: 16 (over y, z), py: 8 (over x, core).
Axes of the slice: x: 4, y: 4, z: 4, core: 2. Of those that a mesh axis runs over, the one named last changes fastest.
Arguments:
- field: bfloat16 [1, 32, 256, 256, 256], P(None, None, 'px', 'py'), may hold values from -6 to 6
- spectral_weight: bfloat16 [2, 32, 32, 32, 64, 64], P(None, None, 'px', 'py'), may hold values from -72 to 72
- point_weight: bfloat16 [32, 32], replicated, may hold values from -1 to 1
- point_bias: float32 [32], replicated, may hold values from -3 to 3
Outputs:
- layer_out: bfloat16 [1, 32, 256, 256, 256], P(None, None, 'px', 'py')
The draws below stay inside these ranges and needn't reach their ends.
All inputs are finite; a program needn't handle non-finite values.
Results may differ from the reference program's by a relative error of at most 0.0085.
Values may be sent and summed in bfloat16 or wider, within the bound.
A program may use at most 192 MiB of HBM per device.

```python
import jax
import jax.numpy as jnp
from jax import lax

C = 32
MX = 64
MY = 64
MZ = 32
NZ = 256
B = 1
NX = 256
NY = 256


def draw_spectral_weight(key, part):
    normal_draw = jnp.clip(jax.random.normal(key, (2, C, C, MZ, MX, MY), jnp.float32), -6.0, 6.0)
    values = 2.0 * normal_draw
    return values.astype(jnp.bfloat16)


def shard_levels(rng, dims, pieces, smallest, largest):
    level = 1.0
    for position, blocks in pieces:
        heights = jax.random.uniform(jax.random.fold_in(jax.random.fold_in(rng, 6), position), (blocks,), jnp.float32, smallest / len(pieces), largest / len(pieces))
        level = level * jnp.repeat(jnp.exp(heights), dims[position] // blocks).reshape((-1,) + (1,) * (len(dims) - 1 - position))
    return level


def scatter_about(stream_key, extent, width, bound, pieces=(), kind=jnp.bfloat16):
    array = width * jax.random.normal(stream_key, extent, jnp.float32)
    if pieces:
        array = array * shard_levels(stream_key, extent, pieces, -0.22, 0.18)
    return jnp.clip(array, -bound, bound).astype(kind)


def setup_inputs(seed: int = 0) -> dict:
    key_of = jax.random.split(jax.random.key(seed), 5)
    field = scatter_about(key_of[0], (B, C, NX, NY, NZ), 1.0, 6.0, ((2, 16), (3, 8)))
    spectral_weight = draw_spectral_weight(jax.random.fold_in(key_of[4], 71), 0)
    point_weight = scatter_about(key_of[2], (C, C), C ** -0.5, 1.0)
    point_bias = scatter_about(key_of[3], (C,), 0.5, 3.0, (), jnp.float32)
    return dict(field=field, spectral_weight=spectral_weight, point_weight=point_weight, point_bias=point_bias)


def contract(form, left, right):
    return jnp.einsum(form, left, right, precision=lax.Precision.HIGHEST, preferred_element_type=jnp.float32)


def reference(field, spectral_weight, point_weight, point_bias):
    batch = field.shape[0]
    channels = field.shape[1]
    index_x = jnp.concatenate([jnp.arange(MX // 2), jnp.arange(NX - MX // 2, NX)]).astype(jnp.int32)
    index_y = jnp.concatenate([jnp.arange(MY // 2), jnp.arange(NY - MY // 2, NY)]).astype(jnp.int32)
    index_z = jnp.arange(MZ).astype(jnp.int32)
    flat = field.reshape(batch * channels, NX, NY, NZ)

    def forward(single):
        full = jnp.fft.rfftn(single.astype(jnp.float32))
        kept = full[index_x][:, index_y][:, :, :MZ]
        return jnp.real(kept), jnp.imag(kept)

    real_all, imag_all = lax.map(forward, flat)
    real_all = jnp.transpose(real_all.reshape(batch, channels, MX, MY, MZ), (0, 1, 4, 2, 3))
    imag_all = jnp.transpose(imag_all.reshape(batch, channels, MX, MY, MZ), (0, 1, 4, 2, 3))
    in_real = lax.optimization_barrier(real_all.astype(jnp.bfloat16)).astype(jnp.float32)
    in_imag = lax.optimization_barrier(imag_all.astype(jnp.bfloat16)).astype(jnp.float32)
    weight_real = spectral_weight[0].astype(jnp.float32)
    weight_imag = spectral_weight[1].astype(jnp.float32)
    mixed_real = contract('bckij,cokij->bokij', in_real, weight_real) - contract('bckij,cokij->bokij', in_imag, weight_imag)
    mixed_imag = contract('bckij,cokij->bokij', in_real, weight_imag) + contract('bckij,cokij->bokij', in_imag, weight_real)
    mixed_real = mixed_real.reshape(batch * channels, MZ, MX, MY)
    mixed_imag = mixed_imag.reshape(batch * channels, MZ, MX, MY)
    weights_f = point_weight.astype(jnp.float32)
    bias_f = point_bias.astype(jnp.float32)

    def inverse(item):
        number, part_real, part_imag = item
        sample = number // channels
        output_channel = number % channels
        placed_real = jnp.zeros((NX, NY, NZ // 2 + 1), part_real.dtype)
        placed_imag = jnp.zeros((NX, NY, NZ // 2 + 1), part_real.dtype)
        spot = (index_x[:, None, None], index_y[None, :, None], index_z[None, None, :])
        placed_real = placed_real.at[spot].set(jnp.transpose(part_real, (1, 2, 0)))
        placed_imag = placed_imag.at[spot].set(jnp.transpose(part_imag, (1, 2, 0)))
        spectral = jnp.fft.irfftn(lax.complex(placed_real, placed_imag), s=(NX, NY, NZ))
        inputs = lax.dynamic_index_in_dim(field, sample, 0, keepdims=False)
        row = lax.dynamic_index_in_dim(weights_f, output_channel, 0, keepdims=False)
        bias_one = lax.dynamic_index_in_dim(bias_f, output_channel, 0, keepdims=False)
        pointwise = jnp.einsum('c,cxyz->xyz', row, inputs.astype(jnp.float32), precision=lax.Precision.HIGHEST) + bias_one
        return jax.nn.gelu(spectral + pointwise, approximate=False).astype(jnp.bfloat16)

    numbers = jnp.arange(batch * channels).astype(jnp.int32)
    result = lax.map(inverse, (numbers, mixed_real, mixed_imag))
    return result.reshape(batch, channels, NX, NY, NZ)
```

```python
import functools

import jax
import jax.numpy as jnp
import ml_dtypes
import numpy as np
from jax import lax
from jax.experimental import pallas as pl
from jax.experimental.pallas import tpu as pltpu
from jax.sharding import PartitionSpec as P

F32 = jnp.float32
BF16 = jnp.bfloat16
MESH = pl.DeviceIdType.MESH
VMEM_LIMIT = 60 * 1024 * 1024


def split_bf16(table):
    high = table.astype(ml_dtypes.bfloat16)
    low = (table - high.astype(np.float64)).astype(ml_dtypes.bfloat16)
    return high, low


def waves(numbers, positions):
    turns = (np.outer(numbers, positions) % 256).astype(np.float64)
    angle = 2.0 * np.pi * turns / 256.0
    return np.cos(angle), np.sin(angle)


def build_tables():
    signed = np.concatenate([np.arange(32), np.arange(32) - 32])
    grid = np.arange(256)
    cos_z, sin_z = waves(np.arange(32), grid)
    z_rows = np.stack([cos_z.reshape(8, 4, 256), -sin_z.reshape(8, 4, 256)], axis=1).reshape(64, 256)
    z_table = np.concatenate(split_bf16(z_rows), axis=0)
    cos_y, sin_y = waves(signed, grid)
    both = np.stack([cos_y, sin_y], axis=0).transpose(2, 0, 1).reshape(8, 32, 2, 64)
    y_table = np.zeros((8, 4, 32, 2, 4, 64))
    for x in range(4):
        y_table[:, x, :, :, x, :] = both
    y_table = y_table.reshape(1024, 512).astype(ml_dtypes.bfloat16)
    r16 = np.arange(16)
    x_of = (16 * np.arange(16)[:, None] + (2 * (r16 % 8) + r16 // 8)[None, :]).reshape(256)
    cos_x, sin_x = waves(signed, x_of)
    x_table = np.concatenate(split_bf16(np.concatenate([cos_x, sin_x], axis=0)), axis=0)
    cos_x, sin_x = waves(signed, grid)
    xi_table = np.concatenate(split_bf16(np.concatenate([cos_x.T, sin_x.T], axis=0)), axis=1)
    c = cos_y.reshape(64, 8, 32)
    s = sin_y.reshape(64, 8, 32)
    yi_table = np.zeros((4, 2, 64, 2, 8, 4, 32))
    for x in range(4):
        yi_table[x, 0, :, 0, :, x, :] = c
        yi_table[x, 1, :, 0, :, x, :] = -s
        yi_table[x, 0, :, 1, :, x, :] = s
        yi_table[x, 1, :, 1, :, x, :] = c
    yi_table = yi_table.reshape(512, 2048).astype(ml_dtypes.bfloat16)
    factor = np.where(np.arange(32) == 0, 1.0, 2.0)[:, None] / 16777216.0
    back = np.stack([(factor * cos_z).reshape(8, 4, 256), (-factor * sin_z).reshape(8, 4, 256)], axis=1)
    zi = np.zeros((8, 2, 2, 4, 2, 256))
    for o in range(2):
        zi[:, :, o, :, o, :] = back
    zi_table = np.concatenate(split_bf16(zi.reshape(128, 512)), axis=0)
    return z_table, y_table, x_table, xi_table, yi_table, zi_table


def dot(a, b):
    return jnp.dot(a, b, preferred_element_type=F32)


def z_forward(field_ref, table_ref, out_ref):
    for c in range(field_ref.shape[0]):
        rows = field_ref[c].reshape(512, 256)
        both = lax.dot_general(
            table_ref[...], rows, (((1,), (1,)), ((), ())), preferred_element_type=F32
        )
        out_ref[:, c] = (both[:64] + both[64:]).reshape(8, 8, 512).astype(BF16)


def y_forward(in_ref, table_ref, out_ref, rows_ref):
    cb = in_ref.shape[1]
    lower = lax.broadcasted_iota(jnp.int32, (cb, 8, 256), 1) < 4
    for quad in range(4):
        left = jnp.concatenate(
            [in_ref[p, :, :, quad * 128 : (quad + 1) * 128].reshape(cb * 8, 128) for p in range(8)],
            axis=1,
        )
        both = dot(left, table_ref[...])
        turned = pltpu.roll(both[:, 256:].reshape(cb, 8, 256), 4, 1)
        value = both[:, :256].reshape(cb, 8, 256) + jnp.where(lower, turned, -turned)
        value = value.reshape(cb * 8, 256)
        rows_ref[pl.ds(2 * quad, cb * 8, stride=8), :] = value[:, :128]
        rows_ref[pl.ds(2 * quad + 1, cb * 8, stride=8), :] = value[:, 128:]
    rows = rows_ref[...].reshape(cb, 2, 4, 8, 128)
    real = rows[:, 0].reshape(cb * 32, 128)
    imag = rows[:, 1].reshape(cb * 32, 128)
    first = lax.broadcasted_iota(jnp.int32, (cb * 32, 128), 1) < 64
    even = jnp.where(first, real, pltpu.roll(imag, 64, 1)).reshape(cb, 4, 8, 128)
    odd = jnp.where(first, pltpu.roll(real, 64, 1), imag).reshape(cb, 4, 8, 128)
    out_ref[...] = jnp.concatenate([even, odd], axis=2).astype(BF16).reshape(out_ref.shape)


def x_forward(in_ref, table_ref, out_ref):
    first = lax.broadcasted_iota(jnp.int32, (64, 128), 1) < 64
    for c in range(2):
        for l in range(4):
            both = dot(table_ref[...], in_ref[:, c, l].reshape(256, 128))
            both = both[:128] + both[128:]
            turned = pltpu.roll(both[64:], 64, 1)
            out_ref[c, l] = (both[:64] + jnp.where(first, turned, -turned)).astype(BF16)


def mix_channels(spec_ref, weight_ref, l):
    def step(c, sums):
        value = spec_ref[c // 2, c % 2, l].astype(F32)
        real = value[:, :64]
        imag = pltpu.roll(value, 64, 1)[:, :64]
        out = []
        for o in range(2):
            wr = weight_ref[0, c, o, l].astype(F32)
            wi = weight_ref[1, c, o, l].astype(F32)
            out.append(sums[2 * o] + (real * wr - imag * wi))
            out.append(sums[2 * o + 1] + (real * wi + imag * wr))
        return tuple(out)

    zero = jnp.zeros((64, 64), F32)
    return lax.fori_loop(0, 32, step, (zero,) * 4)


def x_inverse(spec_ref, weight_ref, table_ref, out_ref, rows_ref):
    first = lax.broadcasted_iota(jnp.int32, (256, 128), 1) < 64
    for l in range(4):
        sums = mix_channels(spec_ref, weight_ref, l)
        for o in range(2):
            mixed = jnp.concatenate([sums[2 * o], sums[2 * o + 1]], axis=1).astype(BF16)
            both = dot(table_ref[...], jnp.concatenate([mixed, mixed], axis=0))
            turned = pltpu.roll(both[256:], 64, 1)
            value = both[:256] + jnp.where(first, -turned, turned)
            rows_ref[pl.ds(o * 4 + l, 256, stride=8), :] = value
    out_ref[...] = rows_ref[...].astype(BF16).reshape(out_ref.shape)


def y_inverse(in_ref, table_ref, out_ref):
    for quad in range(4):
        left = jnp.concatenate(
            [in_ref[:, (quad * 4 + x) * 8 : (quad * 4 + x + 1) * 8, :].reshape(128, 128) for x in range(4)],
            axis=1,
        )
        for ri in range(2):
            value = dot(left, table_ref[:, ri * 1024 : (ri + 1) * 1024]).reshape(16, 8, 1024).astype(BF16)
            for q in range(8):
                out_ref[q, :, ri, :, quad * 128 : (quad + 1) * 128] = value[:, :, q * 128 : (q + 1) * 128]


def finish(field_ref, spec_ref, point_ref, bias_ref, table_ref, out_ref, point_out):
    for x in range(4):
        for y in range(4):
            rows = field_ref[:, x, y * 8 : (y + 1) * 8, :].reshape(256, 256)
            value = dot(point_ref[...], rows) + bias_ref[...]
            point_out[:, x, y * 8 : (y + 1) * 8, :] = value.reshape(32, 8, 256)

    def step(pair, carry):
        g = spec_ref[:, pair].reshape(128, 128)
        value = lax.dot_general(
            jnp.concatenate([g, g], axis=0),
            table_ref[...],
            (((0,), (0,)), ((), ())),
            preferred_element_type=F32,
        )
        for o in range(2):
            total = value[:, o * 256 : (o + 1) * 256].reshape(4, 32, 256) + point_out[2 * pair + o]
            total = 0.5 * total * (1.0 + lax.erf(total * 0.7071067811865476))
            out_ref[2 * pair + o] = total.astype(BF16)
        return carry

    lax.fori_loop(0, 16, step, 0)


def exchange_kernel(axis, size, gather, in_ref, out_ref, send_sem, recv_sem):
    me = lax.axis_index(axis)
    barrier = pltpu.get_barrier_semaphore()
    for d in range(1, size):
        peer = lax.rem(me + d, size)
        pl.semaphore_signal(barrier, inc=1, device_id={axis: peer}, device_id_type=MESH)
    pl.semaphore_wait(barrier, size - 1)

    def copy(d, peer, slot):
        return pltpu.make_async_remote_copy(
            src_ref=in_ref if gather else in_ref.at[peer],
            dst_ref=out_ref.at[slot],
            send_sem=send_sem.at[d],
            recv_sem=recv_sem.at[d],
            device_id={axis: peer},
            device_id_type=MESH,
        )

    for d in range(1, size):
        copy(d, lax.rem(me + d, size), me).start()
    out_ref[me] = in_ref[...] if gather else in_ref[me]
    for d in range(1, size):
        copy(d, lax.rem(me + d, size), lax.rem(me + size - d, size)).wait()


def exchange(value, axis, size, gather, number):
    shape = (size, *value.shape) if gather else value.shape
    return pl.pallas_call(
        functools.partial(exchange_kernel, axis, size, gather),
        out_shape=jax.ShapeDtypeStruct(shape, value.dtype),
        in_specs=[pl.BlockSpec(memory_space=pltpu.VMEM)],
        out_specs=pl.BlockSpec(memory_space=pltpu.VMEM),
        scratch_shapes=[pltpu.SemaphoreType.DMA((size,)), pltpu.SemaphoreType.DMA((size,))],
        compiler_params=pltpu.CompilerParams(
            collective_id=number, has_side_effects=True, vmem_limit_bytes=VMEM_LIMIT
        ),
        name=f"exchange{number}",
    )(value)


def whole(kernel, out_shape, *args, scratch=(), name=None):
    vm = pl.BlockSpec(memory_space=pltpu.VMEM)
    return pl.pallas_call(
        kernel,
        out_shape=jax.ShapeDtypeStruct(out_shape, BF16),
        in_specs=[vm] * len(args),
        out_specs=vm,
        scratch_shapes=list(scratch),
        compiler_params=pltpu.CompilerParams(vmem_limit_bytes=VMEM_LIMIT),
        name=name,
    )(*args)


def body(tables, field, spectral_weight, point_weight, point_bias):
    z_table, y_table, x_table, xi_table, yi_table, zi_table = tables
    field = field.reshape(32, 16, 32, 256)
    along_z = pl.pallas_call(
        z_forward,
        grid=(8,),
        out_shape=jax.ShapeDtypeStruct((8, 32, 8, 512), BF16),
        in_specs=[
            pl.BlockSpec((4, 16, 32, 256), lambda c: (c, 0, 0, 0)),
            pl.BlockSpec((128, 256), lambda c: (0, 0)),
        ],
        out_specs=pl.BlockSpec((8, 4, 8, 512), lambda c: (0, c, 0, 0)),
        compiler_params=pltpu.CompilerParams(vmem_limit_bytes=VMEM_LIMIT),
        name="z_forward",
    )(field, z_table)
    moved = exchange(along_z, "py", 8, False, 1)
    along_y = pl.pallas_call(
        y_forward,
        grid=(4,),
        out_shape=jax.ShapeDtypeStruct((16, 2, 4, 16, 128), BF16),
        in_specs=[
            pl.BlockSpec((8, 8, 8, 512), lambda c: (0, c, 0, 0)),
            pl.BlockSpec((1024, 512), lambda c: (0, 0)),
        ],
        out_specs=pl.BlockSpec((4, 2, 4, 16, 128), lambda c: (c, 0, 0, 0, 0)),
        scratch_shapes=[pltpu.VMEM((512, 128), F32)],
        compiler_params=pltpu.CompilerParams(vmem_limit_bytes=VMEM_LIMIT),
        name="y_forward",
    )(moved, y_table)
    moved = exchange(along_y, "px", 16, False, 2)
    spectrum = whole(x_forward, (2, 4, 64, 128), moved, x_table, name="x_forward")
    gathered = exchange(spectrum, "px", 16, True, 3)
    mixed = whole(
        x_inverse,
        (16, 128, 128),
        gathered,
        spectral_weight,
        xi_table,
        scratch=[pltpu.VMEM((2048, 128), F32)],
        name="x_inverse",
    )
    moved = exchange(mixed, "px", 16, False, 4)
    back = whole(y_inverse, (8, 16, 2, 8, 512), moved, yi_table, name="y_inverse")
    moved = exchange(back, "py", 8, False, 5)
    point = jnp.kron(point_weight.astype(F32), jnp.eye(8, dtype=F32)).astype(BF16)
    bias = jnp.repeat(point_bias, 8)[:, None]
    out = pl.pallas_call(
        finish,
        grid=(4,),
        out_shape=jax.ShapeDtypeStruct((32, 16, 32, 256), BF16),
        in_specs=[
            pl.BlockSpec((32, 4, 32, 256), lambda x: (0, x, 0, 0)),
            pl.BlockSpec((8, 16, 2, 8, 128), lambda x: (0, 0, 0, 0, x)),
            pl.BlockSpec((256, 256), lambda x: (0, 0)),
            pl.BlockSpec((256, 1), lambda x: (0, 0)),
            pl.BlockSpec((256, 512), lambda x: (0, 0)),
        ],
        out_specs=pl.BlockSpec((32, 4, 32, 256), lambda x: (0, x, 0, 0)),
        scratch_shapes=[pltpu.VMEM((32, 4, 32, 256), F32)],
        compiler_params=pltpu.CompilerParams(vmem_limit_bytes=VMEM_LIMIT),
        name="finish",
    )(field, moved, point, bias, zi_table)
    return out.reshape(1, 32, 16, 32, 256)


def solution(mesh):
    tables = tuple(jnp.asarray(t) for t in build_tables())

    def run(field, spectral_weight, point_weight, point_bias):
        return jax.shard_map(
            body,
            mesh=mesh,
            in_specs=((P(),) * 6, P(None, None, "px", "py", None), P(None, None, "px", "py", None, None), P(), P()),
            out_specs=P(None, None, "px", "py", None),
            check_vma=False,
        )(tables, field, spectral_weight, point_weight, point_bias)

    return run
```

```python
import functools

import jax
import jax.numpy as jnp
import ml_dtypes
import numpy as np
from jax import lax
from jax.experimental import pallas as pl
from jax.experimental.pallas import tpu as pltpu
from jax.sharding import PartitionSpec as P

F32 = jnp.float32
BF16 = jnp.bfloat16
MESH = pl.DeviceIdType.MESH
VMEM_LIMIT = 60 * 1024 * 1024


def split_bf16(table):
    high = table.astype(ml_dtypes.bfloat16)
    low = (table - high.astype(np.float64)).astype(ml_dtypes.bfloat16)
    return high, low


def waves(numbers, positions):
    turns = (np.outer(numbers, positions) % 256).astype(np.float64)
    angle = 2.0 * np.pi * turns / 256.0
    return np.cos(angle), np.sin(angle)


def build_tables():
    signed = np.concatenate([np.arange(32), np.arange(32) - 32])
    grid = np.arange(256)
    cos_z, sin_z = waves(np.arange(32), grid)
    z_rows = np.stack([cos_z.reshape(8, 4, 256), -sin_z.reshape(8, 4, 256)], axis=1).reshape(64, 256)
    z_table = np.concatenate(split_bf16(z_rows), axis=0)
    cos_y, sin_y = waves(signed, grid)
    both = np.stack([cos_y, sin_y], axis=0).transpose(2, 0, 1).reshape(8, 32, 2, 64)
    y_table = np.zeros((8, 4, 32, 2, 4, 64))
    for x in range(4):
        y_table[:, x, :, :, x, :] = both
    y_table = y_table.reshape(1024, 512).astype(ml_dtypes.bfloat16)
    r16 = np.arange(16)
    x_of = (16 * np.arange(16)[:, None] + (2 * (r16 % 8) + r16 // 8)[None, :]).reshape(256)
    cos_x, sin_x = waves(signed, x_of)
    x_table = np.concatenate(split_bf16(np.concatenate([cos_x, sin_x], axis=0)), axis=0)
    cos_x, sin_x = waves(signed, grid)
    xi_table = np.concatenate(split_bf16(np.concatenate([cos_x.T, sin_x.T], axis=0)), axis=1)
    c = cos_y.reshape(64, 8, 32)
    s = sin_y.reshape(64, 8, 32)
    yi_table = np.zeros((4, 2, 64, 2, 8, 4, 32))
    for x in range(4):
        yi_table[x, 0, :, 0, :, x, :] = c
        yi_table[x, 1, :, 0, :, x, :] = -s
        yi_table[x, 0, :, 1, :, x, :] = s
        yi_table[x, 1, :, 1, :, x, :] = c
    yi_table = yi_table.reshape(512, 2048).astype(ml_dtypes.bfloat16)
    factor = np.where(np.arange(32) == 0, 1.0, 2.0)[:, None] / 16777216.0
    back = np.stack([(factor * cos_z).reshape(8, 4, 256), (-factor * sin_z).reshape(8, 4, 256)], axis=1)
    zi = np.zeros((8, 2, 2, 4, 2, 256))
    for o in range(2):
        zi[:, :, o, :, o, :] = back
    zi_table = np.concatenate(split_bf16(zi.reshape(128, 512)), axis=0)
    return z_table, y_table, x_table, xi_table, yi_table, zi_table


def dot(a, b):
    return jnp.dot(a, b, preferred_element_type=F32)


def z_group(field_ref, table_ref, out_ref, group):
    for c in range(4):
        rows = field_ref[group * 4 + c].reshape(512, 256)
        both = lax.dot_general(
            table_ref[...], rows, (((1,), (1,)), ((), ())), preferred_element_type=F32
        )
        out_ref[:, group * 4 + c] = (both[:64] + both[64:]).reshape(8, 8, 512).astype(BF16)


def y_group(in_ref, table_ref, out_ref, rows_ref, group):
    part = pl.ds(group * 4, 4)
    left = jnp.concatenate(
        [
            jnp.concatenate(
                [in_ref[p, part, :, quad * 128 : (quad + 1) * 128].reshape(32, 128) for p in range(8)],
                axis=1,
            )
            for quad in range(4)
        ],
        axis=0,
    )
    both = dot(left, table_ref[...])
    turned = pltpu.roll(both[:, 256:].reshape(16, 8, 256), 4, 1)
    lower = lax.broadcasted_iota(jnp.int32, (16, 8, 256), 1) < 4
    value = both[:, :256].reshape(16, 8, 256) + jnp.where(lower, turned, -turned)
    value = value.reshape(128, 256)
    for quad in range(4):
        rows_ref[pl.ds(2 * quad, 32, stride=8), :] = value[quad * 32 : (quad + 1) * 32, :128]
        rows_ref[pl.ds(2 * quad + 1, 32, stride=8), :] = value[quad * 32 : (quad + 1) * 32, 128:]
    rows = rows_ref[...].reshape(4, 2, 4, 8, 128)
    real = rows[:, 0].reshape(128, 128)
    imag = rows[:, 1].reshape(128, 128)
    first = lax.broadcasted_iota(jnp.int32, (128, 128), 1) < 64
    even = jnp.where(first, real, pltpu.roll(imag, 64, 1)).reshape(4, 4, 8, 128)
    odd = jnp.where(first, pltpu.roll(real, 64, 1), imag).reshape(4, 4, 8, 128)
    out_ref[pl.ds(group * 2, 2)] = (
        jnp.concatenate([even, odd], axis=2).astype(BF16).reshape(2, 2, 4, 16, 128)
    )


def x_forward(in_ref, table_ref, out_ref, me):
    first = lax.broadcasted_iota(jnp.int32, (64, 128), 1) < 64
    for c in range(2):
        for l in range(4):
            both = dot(table_ref[...], in_ref[:, c, l].reshape(256, 128))
            both = both[:128] + both[128:]
            turned = pltpu.roll(both[64:], 64, 1)
            out_ref[me, c, l] = (both[:64] + jnp.where(first, turned, -turned)).astype(BF16)


def mix_channel(spec_ref, weight_ref, sum_ref, p, h, fresh=False):
    c = 2 * p + h
    for l in range(4):
        value = spec_ref[p, h, l].astype(F32)
        real = value[:, :64]
        imag = pltpu.roll(value, 64, 1)[:, :64]
        for o in range(2):
            wr = weight_ref[0, c, o, l].astype(F32)
            wi = weight_ref[1, c, o, l].astype(F32)
            mr = real * wr - imag * wi
            mi = real * wi + imag * wr
            if fresh:
                sum_ref[o, l, 0] = mr
                sum_ref[o, l, 1] = mi
            else:
                sum_ref[o, l, 0] += mr
                sum_ref[o, l, 1] += mi


def x_inverse(sum_ref, table_ref, out_ref, rows_ref):
    first = lax.broadcasted_iota(jnp.int32, (256, 128), 1) < 64
    for o in range(2):
        for l in range(4):
            mixed = jnp.concatenate([sum_ref[o, l, 0], sum_ref[o, l, 1]], axis=1).astype(BF16)
            both = dot(table_ref[...], jnp.concatenate([mixed, mixed], axis=0))
            turned = pltpu.roll(both[256:], 64, 1)
            rows_ref[pl.ds(o * 4 + l, 256, stride=8), :] = both[:256] + jnp.where(first, -turned, turned)
    out_ref[...] = rows_ref[...].astype(BF16).reshape(out_ref.shape)


def y_inverse(in_ref, table_ref, out_ref, group):
    part = pl.ds(group * 4, 4)
    left = jnp.concatenate(
        [
            jnp.concatenate(
                [in_ref[part, (quad * 4 + x) * 8 : (quad * 4 + x + 1) * 8, :].reshape(32, 128) for x in range(4)],
                axis=1,
            )
            for quad in range(4)
        ],
        axis=0,
    )
    for ri in range(2):
        value = dot(left, table_ref[:, ri * 1024 : (ri + 1) * 1024]).reshape(4, 4, 8, 1024).astype(BF16)
        for q in range(8):
            for quad in range(4):
                out_ref[q, part, ri, :, quad * 128 : (quad + 1) * 128] = value[quad, :, :, q * 128 : (q + 1) * 128]


def transform(
    field_hbm, weight_hbm, zt_hbm, yt_hbm, xt_hbm, xit_hbm, yit_hbm, out_hbm,
    field, weight, zt, yt, xt, xit, yit,
    z_out, y_in, y_rows, y_out, x_in, spec, sums, m_rows, m_out, b_in, b_out,
    load_sem, field_sem, s1, r1, s2, r2, s3, r3, s4, r4, s5, r5, own_sem,
):
    px = lax.axis_index("px")
    py = lax.axis_index("py")
    row = px // 4
    col = lax.rem(px, 4)

    def wrap(value, size):
        return lax.rem(value + size, size)

    first_group = wrap(px // 2 + 1, 8)

    def channel_group(step):
        return wrap(first_group + step, 8)

    def load_field(step):
        part = pl.ds(channel_group(step) * 4, 4)
        return pltpu.make_async_copy(field_hbm.at[part], field.at[part], field_sem.at[step])

    loads = [
        pltpu.make_async_copy(a, b, load_sem.at[n])
        for n, (a, b) in enumerate(
            ((zt_hbm, zt), (yt_hbm, yt), (xt_hbm, xt), (weight_hbm, weight), (xit_hbm, xit), (yit_hbm, yit))
        )
    ]
    loads[0].start()
    for step in range(8):
        load_field(step).start()
    for load in loads[1:]:
        load.start()

    barrier = pltpu.get_barrier_semaphore()
    for d in range(1, 8):
        pl.semaphore_signal(barrier, inc=1, device_id={"py": wrap(py + d, 8)}, device_id_type=MESH)
    for d in range(1, 16):
        pl.semaphore_signal(barrier, inc=1, device_id={"px": wrap(px + d, 16)}, device_id_type=MESH)

    def remote(src, dst, send, recv, axis, peer):
        return pltpu.make_async_remote_copy(
            src_ref=src, dst_ref=dst, send_sem=send, recv_sem=recv, device_id={axis: peer}, device_id_type=MESH
        )

    def send1(step, d, slot):
        part = pl.ds(channel_group(step) * 4, 4)
        peer = wrap(py + d, 8)
        return remote(z_out.at[peer, part], y_in.at[slot, part], s1.at[step, d], r1.at[step, d], "py", peer)

    def do_z(step):
        load_field(step).wait()
        group = channel_group(step)
        z_group(field, zt, z_out, group)
        y_in[py, pl.ds(group * 4, 4)] = z_out[py, pl.ds(group * 4, 4)]

    def send_z(step):
        for d in range(1, 8):
            send1(step, d, py).start()

    loads[0].wait()
    do_z(0)
    pl.semaphore_wait(barrier, 22)
    send_z(0)

    def z_step(step, carry):
        do_z(step)
        send_z(step)
        return carry

    lax.fori_loop(1, 8, z_step, 0)

    def send2(peer, slot, d):
        return remote(y_out.at[peer], x_in.at[slot], s2.at[d], r2.at[d], "px", peer)

    loads[1].wait()

    def y_step(step, carry):
        for d in range(1, 8):
            send1(step, d, wrap(py - d, 8)).wait_recv()
        group = channel_group(step)
        y_group(y_in, yt, y_out, y_rows, group)
        for half in range(2):
            peer = 2 * group + half

            @pl.when(peer != px)
            def _():
                send2(peer, px, wrap(peer - px, 16)).start()

        return carry

    lax.fori_loop(0, 8, y_step, 0)
    x_in[px] = y_out[px]
    for d in range(1, 16):
        send2(wrap(px + d, 16), wrap(px - d, 16), d).wait_recv()

    loads[2].wait()
    x_forward(x_in, xt, spec, px)
    loads[3].wait()

    def block(h, a, b):
        r, c = (b, a) if h == 0 else (a, b)
        return 4 * wrap(r, 4) + wrap(c, 4)

    near = [(col, row), (row, col)]
    steps = (0, -1, 1, 2)
    parts = (slice(0, 4), slice(0, 4), slice(0, 2), slice(2, 4))

    def first_phase(h, kind, receiving):
        a, b = near[h]
        sign = 1 if kind in (0, 2) else -1
        origin = (0, 0, -1, 1)[kind] - (sign if receiving else 0)
        place = spec.at[block(h, a + origin, b), h, parts[kind]]
        n = h * 20 + kind
        return remote(place, place, s3.at[n], r3.at[n], "px", block(h, a + sign, b))

    def second_phase(h, k, kind, receiving):
        a, b = near[h]
        sign = 1 if kind in (0, 2) else -1
        origin = (0, 0, -1, 1)[kind] - (sign if receiving else 0)
        place = spec.at[block(h, a + steps[k], b + origin), h, parts[kind]]
        n = h * 20 + 4 + 4 * k + kind
        return remote(place, place, s3.at[n], r3.at[n], "px", block(h, a, b + sign))

    def mix(h, da, db, fresh=False):
        a, b = near[h]
        mix_channel(spec, weight, sums, block(h, a + da, b + db), h, fresh)

    for h in range(2):
        for kind in range(2):
            first_phase(h, kind, False).start()
    for h in range(2):
        for kind in range(2):
            second_phase(h, 0, kind, False).start()
    mix(0, 0, 0, True)
    mix(1, 0, 0)
    for kind in range(2):
        for h in range(2):
            first_phase(h, kind, True).wait_recv()
            first_phase(h, kind + 2, False).start()
            for other in range(2):
                second_phase(h, kind + 1, other, False).start()
    for h in range(2):
        mix(h, -1, 0)
        mix(h, 1, 0)
    for h in range(2):
        for kind in (2, 3):
            first_phase(h, kind, True).wait_recv()
        for other in range(2):
            second_phase(h, 3, other, False).start()
    for h in range(2):
        mix(h, 2, 0)
    for k in range(4):
        for h in range(2):
            for kind in range(2):
                second_phase(h, k, kind, True).wait_recv()
                second_phase(h, k, kind + 2, False).start()
        for h in range(2):
            mix(h, steps[k], -1)
            mix(h, steps[k], 1)
    for k in range(4):
        for h in range(2):
            for kind in (2, 3):
                second_phase(h, k, kind, True).wait_recv()
            mix(h, steps[k], 2)

    loads[4].wait()
    x_inverse(sums, xit, m_out, m_rows)

    def send4(peer, slot, d):
        return remote(m_out.at[peer], b_in.at[slot], s4.at[d], r4.at[d], "px", peer)

    rows_order = (0, 1, 3, 2)
    for dr in rows_order:
        for dc in range(4):
            if dr or dc:
                peer = 4 * wrap(row - dr, 4) + wrap(col - dc, 4)
                send4(peer, px, 4 * dr + dc).start()
    b_in[px] = m_out[px]

    def send5(dr, d, slot):
        part = pl.ds(4 * wrap(row + dr, 4), 4)
        peer = wrap(py + d, 8)
        return remote(b_out.at[peer, part], out_hbm.at[slot, part], s5.at[dr, d], r5.at[dr, d], "py", peer)

    loads[5].wait()
    for dr in rows_order:
        for dc in range(4):
            if dr or dc:
                source = 4 * wrap(row + dr, 4) + wrap(col + dc, 4)
                send4(source, source, 4 * dr + dc).wait_recv()
        y_inverse(b_in, yit, b_out, wrap(row + dr, 4))
        for d in range(1, 8):
            send5(dr, d, py).start()
    own = pltpu.make_async_copy(b_out.at[py], out_hbm.at[py], own_sem)
    own.start()

    for dr in rows_order:
        for d in range(1, 8):
            send5(dr, d, wrap(py - d, 8)).wait_recv()
    own.wait()

    def drain(step, carry):
        for d in range(1, 8):
            send1(step, d, py).wait_send()
        return carry

    lax.fori_loop(0, 8, drain, 0)
    for d in range(1, 16):
        send2(wrap(px + d, 16), px, d).wait_send()
    for h in range(2):
        for kind in range(4):
            first_phase(h, kind, False).wait_send()
            for k in range(4):
                second_phase(h, k, kind, False).wait_send()
    for dr in range(4):
        for dc in range(4):
            if dr or dc:
                send4(4 * wrap(row - dr, 4) + wrap(col - dc, 4), px, 4 * dr + dc).wait_send()
        for d in range(1, 8):
            send5(dr, d, py).wait_send()


def finish(field_ref, spec_ref, point_ref, bias_ref, table_ref, out_ref, point_out, spread):
    @pl.when(pl.program_id(0) == 0)
    def _():
        r = lax.broadcasted_iota(jnp.int32, (256, 32), 0)
        c = lax.broadcasted_iota(jnp.int32, (256, 32), 1)
        tall = ((r >= 8 * c) & (r < 8 * c + 8)).astype(F32).astype(BF16)
        r = lax.broadcasted_iota(jnp.int32, (32, 256), 0)
        c = lax.broadcasted_iota(jnp.int32, (32, 256), 1)
        wide = ((c >= 8 * r) & (c < 8 * r + 8)).astype(F32).astype(BF16)
        r = lax.broadcasted_iota(jnp.int32, (256, 256), 0)
        c = lax.broadcasted_iota(jnp.int32, (256, 256), 1)
        every = dot(dot(tall, point_ref[...]).astype(BF16), wide)
        spread[...] = jnp.where((r & 7) == (c & 7), every, 0.0).astype(BF16)

    for x in range(4):
        for y in range(4):
            rows = field_ref[:, x, y * 8 : (y + 1) * 8, :].reshape(256, 256)
            point_out[:, x, y * 8 : (y + 1) * 8, :] = dot(spread[...], rows).reshape(32, 8, 256)

    def step(pair, carry):
        g = spec_ref[:, pair].reshape(128, 128)
        value = lax.dot_general(
            jnp.concatenate([g, g], axis=0),
            table_ref[...],
            (((0,), (0,)), ((), ())),
            preferred_element_type=F32,
        )
        for o in range(2):
            total = value[:, o * 256 : (o + 1) * 256].reshape(4, 32, 256) + point_out[2 * pair + o]
            total = total + bias_ref[2 * pair + o]
            total = 0.5 * total * (1.0 + lax.erf(total * 0.7071067811865476))
            out_ref[2 * pair + o] = total.astype(BF16)
        return carry

    lax.fori_loop(0, 16, step, 0)


def body(tables, field, spectral_weight, point_weight, point_bias):
    z_table, y_table, x_table, xi_table, yi_table, zi_table = tables
    field = field.reshape(32, 16, 32, 256)
    anywhere = pl.BlockSpec(memory_space=pl.ANY)
    dma = pltpu.SemaphoreType.DMA
    operands = (field, spectral_weight, z_table, y_table, x_table, xi_table, yi_table)
    spectral = pl.pallas_call(
        transform,
        out_shape=jax.ShapeDtypeStruct((8, 16, 2, 8, 512), BF16),
        in_specs=[anywhere] * len(operands),
        out_specs=anywhere,
        scratch_shapes=[
            *[pltpu.VMEM(a.shape, a.dtype) for a in operands],
            pltpu.VMEM((8, 32, 8, 512), BF16),
            pltpu.VMEM((8, 32, 8, 512), BF16),
            pltpu.VMEM((256, 128), F32),
            pltpu.VMEM((16, 2, 4, 16, 128), BF16),
            pltpu.VMEM((16, 2, 4, 16, 128), BF16),
            pltpu.VMEM((16, 2, 4, 64, 128), BF16),
            pltpu.VMEM((2, 4, 2, 64, 64), F32),
            pltpu.VMEM((2048, 128), F32),
            pltpu.VMEM((16, 128, 128), BF16),
            pltpu.VMEM((16, 128, 128), BF16),
            pltpu.VMEM((8, 16, 2, 8, 512), BF16),
            dma((6,)), dma((8,)),
            dma((8, 8)), dma((8, 8)),
            dma((16,)), dma((16,)),
            dma((40,)), dma((40,)),
            dma((16,)), dma((16,)),
            dma((4, 8)), dma((4, 8)),
            dma,
        ],
        compiler_params=pltpu.CompilerParams(
            collective_id=1, has_side_effects=True, vmem_limit_bytes=VMEM_LIMIT
        ),
        name="transform",
    )(*operands)
    out = pl.pallas_call(
        finish,
        grid=(4,),
        out_shape=jax.ShapeDtypeStruct((32, 16, 32, 256), BF16),
        in_specs=[
            pl.BlockSpec((32, 4, 32, 256), lambda x: (0, x, 0, 0)),
            pl.BlockSpec((8, 16, 2, 8, 128), lambda x: (0, 0, 0, 0, x)),
            pl.BlockSpec((32, 32), lambda x: (0, 0)),
            pl.BlockSpec(memory_space=pltpu.SMEM),
            pl.BlockSpec((256, 512), lambda x: (0, 0)),
        ],
        out_specs=pl.BlockSpec((32, 4, 32, 256), lambda x: (0, x, 0, 0)),
        scratch_shapes=[pltpu.VMEM((32, 4, 32, 256), F32), pltpu.VMEM((256, 256), BF16)],
        compiler_params=pltpu.CompilerParams(vmem_limit_bytes=VMEM_LIMIT),
        name="finish",
    )(field, spectral, point_weight, point_bias, zi_table)
    return out.reshape(1, 32, 16, 32, 256)


def solution(mesh):
    tables = tuple(jnp.asarray(t) for t in build_tables())

    def run(field, spectral_weight, point_weight, point_bias):
        return jax.shard_map(
            body,
            mesh=mesh,
            in_specs=((P(),) * 6, P(None, None, "px", "py", None), P(None, None, "px", "py", None, None), P(), P()),
            out_specs=P(None, None, "px", "py", None),
            check_vma=False,
        )(tables, field, spectral_weight, point_weight, point_bias)

    return run
```

```python
import functools

import jax
import jax.numpy as jnp
import ml_dtypes
import numpy as np
from jax import lax
from jax.experimental import pallas as pl
from jax.experimental.pallas import tpu as pltpu
from jax.sharding import PartitionSpec as P

F32 = jnp.float32
BF16 = jnp.bfloat16
MESH = pl.DeviceIdType.MESH
VMEM_LIMIT = 60 * 1024 * 1024


def split_bf16(table):
    high = table.astype(ml_dtypes.bfloat16)
    low = (table - high.astype(np.float64)).astype(ml_dtypes.bfloat16)
    return high, low


def waves(numbers, positions):
    turns = (np.outer(numbers, positions) % 256).astype(np.float64)
    angle = 2.0 * np.pi * turns / 256.0
    return np.cos(angle), np.sin(angle)


def build_tables():
    signed = np.concatenate([np.arange(32), np.arange(32) - 32])
    grid = np.arange(256)
    cos_z, sin_z = waves(np.arange(32), grid)
    z_rows = np.stack([cos_z.reshape(8, 4, 256), -sin_z.reshape(8, 4, 256)], axis=1).reshape(64, 256)
    z_table = np.concatenate(split_bf16(z_rows), axis=0)
    cos_y, sin_y = waves(signed, grid)
    both = np.stack([cos_y, sin_y], axis=0).transpose(2, 0, 1).reshape(8, 32, 2, 64)
    y_table = np.zeros((8, 4, 32, 2, 4, 64))
    for x in range(4):
        y_table[:, x, :, :, x, :] = both
    y_table = y_table.reshape(1024, 512).astype(ml_dtypes.bfloat16)
    r16 = np.arange(16)
    x_of = (16 * np.arange(16)[:, None] + (2 * (r16 % 8) + r16 // 8)[None, :]).reshape(256)
    cos_x, sin_x = waves(signed, x_of)
    x_table = np.concatenate(split_bf16(np.concatenate([cos_x, sin_x], axis=0)), axis=0)
    cos_x, sin_x = waves(signed, grid)
    xi_table = np.concatenate(split_bf16(np.concatenate([cos_x.T, sin_x.T], axis=0)), axis=1)
    c = cos_y.reshape(64, 8, 32)
    s = sin_y.reshape(64, 8, 32)
    yi_table = np.zeros((4, 2, 64, 2, 8, 4, 32))
    for x in range(4):
        yi_table[x, 0, :, 0, :, x, :] = c
        yi_table[x, 1, :, 0, :, x, :] = -s
        yi_table[x, 0, :, 1, :, x, :] = s
        yi_table[x, 1, :, 1, :, x, :] = c
    yi_table = yi_table.reshape(512, 2048).astype(ml_dtypes.bfloat16)
    factor = np.where(np.arange(32) == 0, 1.0, 2.0)[:, None] / 16777216.0
    back = np.stack([(factor * cos_z).reshape(8, 4, 256), (-factor * sin_z).reshape(8, 4, 256)], axis=1)
    zi = np.zeros((8, 2, 2, 4, 2, 256))
    for o in range(2):
        zi[:, :, o, :, o, :] = back
    zi_table = np.concatenate(split_bf16(zi.reshape(128, 512)), axis=0)
    return z_table, y_table, x_table, xi_table, yi_table, zi_table


def dot(a, b):
    return jnp.dot(a, b, preferred_element_type=F32)


def z_group(field_ref, table_ref, out_ref, group):
    for c in range(4):
        rows = field_ref[group * 4 + c].reshape(512, 256)
        both = lax.dot_general(
            table_ref[...], rows, (((1,), (1,)), ((), ())), preferred_element_type=F32
        )
        out_ref[:, group * 4 + c] = (both[:64] + both[64:]).reshape(8, 8, 512).astype(BF16)


def y_group(in_ref, table_ref, out_ref, rows_ref, group):
    part = pl.ds(group * 4, 4)
    left = jnp.concatenate(
        [
            jnp.concatenate(
                [in_ref[p, part, :, quad * 128 : (quad + 1) * 128].reshape(32, 128) for p in range(8)],
                axis=1,
            )
            for quad in range(4)
        ],
        axis=0,
    )
    both = dot(left, table_ref[...])
    turned = pltpu.roll(both[:, 256:].reshape(16, 8, 256), 4, 1)
    lower = lax.broadcasted_iota(jnp.int32, (16, 8, 256), 1) < 4
    value = both[:, :256].reshape(16, 8, 256) + jnp.where(lower, turned, -turned)
    value = value.reshape(128, 256)
    for quad in range(4):
        rows_ref[pl.ds(2 * quad, 32, stride=8), :] = value[quad * 32 : (quad + 1) * 32, :128]
        rows_ref[pl.ds(2 * quad + 1, 32, stride=8), :] = value[quad * 32 : (quad + 1) * 32, 128:]
    rows = rows_ref[...].reshape(4, 2, 4, 8, 128)
    real = rows[:, 0].reshape(128, 128)
    imag = rows[:, 1].reshape(128, 128)
    first = lax.broadcasted_iota(jnp.int32, (128, 128), 1) < 64
    even = jnp.where(first, real, pltpu.roll(imag, 64, 1)).reshape(4, 4, 8, 128)
    odd = jnp.where(first, pltpu.roll(real, 64, 1), imag).reshape(4, 4, 8, 128)
    out_ref[group] = jnp.concatenate([even, odd], axis=2).astype(BF16).reshape(16, 16, 128)


def x_group(in_ref, table_ref, out_ref, group, row, col):
    both = dot(table_ref[...], in_ref[group].reshape(256, 128))
    both = both[:128] + both[128:]
    turned = pltpu.roll(both[64:], 64, 1)
    first = lax.broadcasted_iota(jnp.int32, (64, 128), 1) < 64
    out_ref[group, row, col] = (both[:64] + jnp.where(first, turned, -turned)).astype(BF16)


def mix_group(spec_ref, weight_ref, sum_ref, group):
    for l in range(4):
        sums = [None] * 4
        for ci in range(4):
            c = 4 * group + ci
            value = spec_ref[group, ci, l].astype(F32)
            real = value[:, :64]
            imag = pltpu.roll(value, 64, 1)[:, :64]
            for o in range(2):
                wr = weight_ref[0, c, o, l].astype(F32)
                wi = weight_ref[1, c, o, l].astype(F32)
                for n, term in enumerate((real * wr - imag * wi, real * wi + imag * wr)):
                    sums[2 * o + n] = term if ci == 0 else sums[2 * o + n] + term
        for o in range(2):
            for n in range(2):
                sum_ref[o, l, n] += sums[2 * o + n]


def x_inverse(sum_ref, table_ref, out_ref, rows_ref):
    first = lax.broadcasted_iota(jnp.int32, (256, 128), 1) < 64
    for o in range(2):
        for l in range(4):
            mixed = jnp.concatenate([sum_ref[o, l, 0], sum_ref[o, l, 1]], axis=1).astype(BF16)
            both = dot(table_ref[...], jnp.concatenate([mixed, mixed], axis=0))
            turned = pltpu.roll(both[256:], 64, 1)
            rows_ref[pl.ds(o * 4 + l, 256, stride=8), :] = both[:256] + jnp.where(first, -turned, turned)
    out_ref[...] = rows_ref[...].astype(BF16).reshape(out_ref.shape)


def y_inverse(in_ref, table_ref, out_ref, group):
    part = pl.ds(group * 4, 4)
    left = jnp.concatenate(
        [
            jnp.concatenate(
                [in_ref[part, (quad * 4 + x) * 8 : (quad * 4 + x + 1) * 8, :].reshape(32, 128) for x in range(4)],
                axis=1,
            )
            for quad in range(4)
        ],
        axis=0,
    )
    for ri in range(2):
        value = dot(left, table_ref[:, ri * 1024 : (ri + 1) * 1024]).reshape(4, 4, 8, 1024).astype(BF16)
        for q in range(8):
            for quad in range(4):
                out_ref[q, part, ri, :, quad * 128 : (quad + 1) * 128] = value[quad, :, :, q * 128 : (q + 1) * 128]


def transform(
    field_hbm, weight_hbm, zt_hbm, yt_hbm, xt_hbm, xit_hbm, yit_hbm, out_hbm,
    field, weight, zt, yt, xt, xit, yit,
    z_out, y_in, y_rows, y_out, x_in, spec, sums, m_rows, m_out, b_in, b_out,
    load_sem, field_sem, s1, r1, s2, r2, s3, r3, s4, r4, s5, r5, own_sem,
):
    px = lax.axis_index("px")
    py = lax.axis_index("py")
    row = px // 4
    col = lax.rem(px, 4)

    def wrap(value, size):
        return lax.rem(value + size, size)

    def load_field(step):
        part = pl.ds(step * 4, 4)
        return pltpu.make_async_copy(field_hbm.at[part], field.at[part], field_sem.at[step])

    loads = [
        pltpu.make_async_copy(a, b, load_sem.at[n])
        for n, (a, b) in enumerate(
            ((zt_hbm, zt), (yt_hbm, yt), (xt_hbm, xt), (weight_hbm, weight), (xit_hbm, xit), (yit_hbm, yit))
        )
    ]
    loads[0].start()
    for step in range(8):
        load_field(step).start()
    for load in loads[1:]:
        load.start()

    barrier = pltpu.get_barrier_semaphore()
    for d in range(1, 8):
        pl.semaphore_signal(barrier, inc=1, device_id={"py": wrap(py + d, 8)}, device_id_type=MESH)
    for d in range(1, 16):
        pl.semaphore_signal(barrier, inc=1, device_id={"px": wrap(px + d, 16)}, device_id_type=MESH)

    def remote(src, dst, send, recv, axis, peer):
        return pltpu.make_async_remote_copy(
            src_ref=src, dst_ref=dst, send_sem=send, recv_sem=recv, device_id={axis: peer}, device_id_type=MESH
        )

    def wait(view, semaphore):
        pltpu.make_async_copy(view, view, semaphore).wait()

    def send1(step, d, slot):
        part = pl.ds(step * 4, 4)
        peer = wrap(py + d, 8)
        return remote(z_out.at[peer, part], y_in.at[slot, part], s1, r1.at[step], "py", peer)

    def do_z(step):
        load_field(step).wait()
        z_group(field, zt, z_out, step)
        y_in[py, pl.ds(step * 4, 4)] = z_out[py, pl.ds(step * 4, 4)]

    def send_z(step):
        for d in range(1, 8):
            send1(step, d, py).start()

    loads[0].wait()
    do_z(0)
    pl.semaphore_wait(barrier, 22)
    send_z(0)

    def z_step(step, carry):
        do_z(step)
        send_z(step)
        return carry

    lax.fori_loop(1, 8, z_step, 0)

    def send2(step, peer, slot):
        return remote(y_out.at[step, peer], x_in.at[step, slot], s2, r2.at[step], "px", peer)

    def do_y(step):
        wait(y_in.at[pl.ds(0, 7), pl.ds(step * 4, 4)], r1.at[step])
        y_group(y_in, yt, y_out, y_rows, step)
        for d in range(1, 16):
            send2(step, wrap(px + d, 16), px).start()
        x_in[step, px] = y_out[step, px]

    halves = (pl.ds(0, 32), pl.ds(32, 32))

    def gather(step, phase, h, d):
        along_col = (h == 0) == (phase == 0)
        if phase == 0:
            place = spec.at[step, row, col, halves[h]]
        elif along_col:
            place = spec.at[step, :, col, halves[h]]
        else:
            place = spec.at[step, row, :, halves[h]]
        peer = 4 * row + wrap(col + d, 4) if along_col else 4 * wrap(row + d, 4) + col
        return remote(place, place, s3, r3.at[step, phase], "px", peer)

    def do_x(step):
        wait(x_in.at[step, pl.ds(0, 15)], r2.at[step])
        x_group(x_in, xt, spec, step, row, col)
        for d in (1, 3, 2):
            for h in range(2):
                gather(step, 0, h, d).start()

    def do_second(step):
        wait(spec.at[step, 0, pl.ds(0, 3)], r3.at[step, 0])
        for h in range(2):
            for d in (1, 3, 2):
                gather(step, 1, h, d).start()

    def do_mix(step):
        wait(spec.at[step, pl.ds(0, 3)], r3.at[step, 1])
        mix_group(spec, weight, sums, step)

    loads[1].wait()
    loads[2].wait()
    loads[3].wait()
    sums[...] = jnp.zeros_like(sums)

    def y_step(step, carry):
        do_y(step)
        pl.when(step >= 1)(lambda: do_x(step - 1))
        pl.when(step >= 2)(lambda: do_second(step - 2))
        pl.when(step >= 5)(lambda: do_mix(step - 5))
        return carry

    lax.fori_loop(0, 8, y_step, 0)
    do_mix(3)
    do_x(7)
    do_second(6)
    do_mix(4)
    do_mix(5)
    do_second(7)
    do_mix(6)
    do_mix(7)

    loads[4].wait()
    x_inverse(sums, xit, m_out, m_rows)

    def send4(peer, slot, d):
        return remote(m_out.at[peer], b_in.at[slot], s4, r4.at[d], "px", peer)

    rows_order = (0, 1, 3, 2)
    for dr in rows_order:
        for dc in range(4):
            if dr or dc:
                peer = 4 * wrap(row - dr, 4) + wrap(col - dc, 4)
                send4(peer, px, dr).start()
    b_in[px] = m_out[px]

    def send5(dr, d, slot):
        part = pl.ds(4 * wrap(row + dr, 4), 4)
        peer = wrap(py + d, 8)
        return remote(b_out.at[peer, part], out_hbm.at[slot, part], s5, r5.at[dr], "py", peer)

    loads[5].wait()
    for dr in rows_order:
        wait(b_in.at[pl.ds(0, 4 if dr else 3)], r4.at[dr])
        y_inverse(b_in, yit, b_out, wrap(row + dr, 4))
        for d in range(1, 8):
            send5(dr, d, py).start()
    own = pltpu.make_async_copy(b_out.at[py], out_hbm.at[py], own_sem)
    own.start()

    for dr in rows_order:
        wait(out_hbm.at[pl.ds(0, 7), pl.ds(4 * dr, 4)], r5.at[dr])
    own.wait()

    wait(z_out.at[pl.ds(0, 7)], s1)
    wait(y_out.at[:, pl.ds(0, 15)], s2)
    wait(spec.at[:, 0, pl.ds(0, 3)], s3)
    wait(spec.at[:, pl.ds(0, 3)], s3)
    wait(m_out.at[pl.ds(0, 15)], s4)
    wait(b_out.at[pl.ds(0, 7)], s5)


def finish(field_ref, spec_ref, point_ref, bias_ref, table_ref, out_ref, point_out, spread):
    @pl.when(pl.program_id(0) == 0)
    def _():
        r = lax.broadcasted_iota(jnp.int32, (256, 32), 0)
        c = lax.broadcasted_iota(jnp.int32, (256, 32), 1)
        tall = ((r >= 8 * c) & (r < 8 * c + 8)).astype(F32).astype(BF16)
        r = lax.broadcasted_iota(jnp.int32, (32, 256), 0)
        c = lax.broadcasted_iota(jnp.int32, (32, 256), 1)
        wide = ((c >= 8 * r) & (c < 8 * r + 8)).astype(F32).astype(BF16)
        r = lax.broadcasted_iota(jnp.int32, (256, 256), 0)
        c = lax.broadcasted_iota(jnp.int32, (256, 256), 1)
        every = dot(dot(tall, point_ref[...]).astype(BF16), wide)
        spread[...] = jnp.where((r & 7) == (c & 7), every, 0.0).astype(BF16)

    for x in range(4):
        for y in range(4):
            rows = field_ref[:, x, y * 8 : (y + 1) * 8, :].reshape(256, 256)
            point_out[:, x, y * 8 : (y + 1) * 8, :] = dot(spread[...], rows).reshape(32, 8, 256)

    def step(pair, carry):
        g = spec_ref[:, pair].reshape(128, 128)
        value = lax.dot_general(
            jnp.concatenate([g, g], axis=0),
            table_ref[...],
            (((0,), (0,)), ((), ())),
            preferred_element_type=F32,
        )
        for o in range(2):
            total = value[:, o * 256 : (o + 1) * 256].reshape(4, 32, 256) + point_out[2 * pair + o]
            total = total + bias_ref[2 * pair + o]
            total = 0.5 * total * (1.0 + lax.erf(total * 0.7071067811865476))
            out_ref[2 * pair + o] = total.astype(BF16)
        return carry

    lax.fori_loop(0, 16, step, 0, unroll=8)


def body(tables, field, spectral_weight, point_weight, point_bias):
    z_table, y_table, x_table, xi_table, yi_table, zi_table = tables
    field = field.reshape(32, 16, 32, 256)
    anywhere = pl.BlockSpec(memory_space=pl.ANY)
    dma = pltpu.SemaphoreType.DMA
    operands = (field, spectral_weight, z_table, y_table, x_table, xi_table, yi_table)
    spectral = pl.pallas_call(
        transform,
        out_shape=jax.ShapeDtypeStruct((8, 16, 2, 8, 512), BF16),
        in_specs=[anywhere] * len(operands),
        out_specs=anywhere,
        scratch_shapes=[
            *[pltpu.VMEM(a.shape, a.dtype) for a in operands],
            pltpu.VMEM((8, 32, 8, 512), BF16),
            pltpu.VMEM((8, 32, 8, 512), BF16),
            pltpu.VMEM((256, 128), F32),
            pltpu.VMEM((8, 16, 16, 128), BF16),
            pltpu.VMEM((8, 16, 16, 128), BF16),
            pltpu.VMEM((8, 4, 4, 64, 128), BF16),
            pltpu.VMEM((2, 4, 2, 64, 64), F32),
            pltpu.VMEM((2048, 128), F32),
            pltpu.VMEM((16, 128, 128), BF16),
            pltpu.VMEM((16, 128, 128), BF16),
            pltpu.VMEM((8, 16, 2, 8, 512), BF16),
            dma((6,)), dma((8,)),
            dma, dma((8,)),
            dma, dma((8,)),
            dma, dma((8, 2)),
            dma, dma((4,)),
            dma, dma((4,)),
            dma,
        ],
        compiler_params=pltpu.CompilerParams(
            collective_id=1, has_side_effects=True, vmem_limit_bytes=VMEM_LIMIT
        ),
        name="transform",
    )(*operands)
    out = pl.pallas_call(
        finish,
        grid=(4,),
        out_shape=jax.ShapeDtypeStruct((32, 16, 32, 256), BF16),
        in_specs=[
            pl.BlockSpec((32, 4, 32, 256), lambda x: (0, x, 0, 0)),
            pl.BlockSpec((8, 16, 2, 8, 128), lambda x: (0, 0, 0, 0, x)),
            pl.BlockSpec((32, 32), lambda x: (0, 0)),
            pl.BlockSpec(memory_space=pltpu.SMEM),
            pl.BlockSpec((256, 512), lambda x: (0, 0)),
        ],
        out_specs=pl.BlockSpec((32, 4, 32, 256), lambda x: (0, x, 0, 0)),
        scratch_shapes=[pltpu.VMEM((32, 4, 32, 256), F32), pltpu.VMEM((256, 256), BF16)],
        compiler_params=pltpu.CompilerParams(vmem_limit_bytes=VMEM_LIMIT),
        name="finish",
    )(field, spectral, point_weight, point_bias, zi_table)
    return out.reshape(1, 32, 16, 32, 256)


def solution(mesh):
    tables = tuple(jnp.asarray(t) for t in build_tables())

    def run(field, spectral_weight, point_weight, point_bias):
        return jax.shard_map(
            body,
            mesh=mesh,
            in_specs=((P(),) * 6, P(None, None, "px", "py", None), P(None, None, "px", "py", None, None), P(), P()),
            out_specs=P(None, None, "px", "py", None),
            check_vma=False,
        )(tables, field, spectral_weight, point_weight, point_bias)

    return run
```

```python
import functools

import jax
import jax.numpy as jnp
import ml_dtypes
import numpy as np
from jax import lax
from jax.experimental import pallas as pl
from jax.experimental.pallas import tpu as pltpu
from jax.sharding import PartitionSpec as P

F32 = jnp.float32
BF16 = jnp.bfloat16
MESH = pl.DeviceIdType.MESH
VMEM_LIMIT = 60 * 1024 * 1024


def split_bf16(table):
    high = table.astype(ml_dtypes.bfloat16)
    low = (table - high.astype(np.float64)).astype(ml_dtypes.bfloat16)
    return high, low


def waves(numbers, positions):
    turns = (np.outer(numbers, positions) % 256).astype(np.float64)
    angle = 2.0 * np.pi * turns / 256.0
    return np.cos(angle), np.sin(angle)


def build_tables():
    signed = np.concatenate([np.arange(32), np.arange(32) - 32])
    grid = np.arange(256)
    cos_z, sin_z = waves(np.arange(32), grid)
    z_rows = np.stack([cos_z.reshape(8, 4, 256), -sin_z.reshape(8, 4, 256)], axis=1).reshape(64, 256)
    z_table = np.concatenate(split_bf16(z_rows), axis=0)
    cos_y, sin_y = waves(signed, grid)
    both = np.stack([cos_y, sin_y], axis=0).transpose(2, 0, 1).reshape(8, 32, 2, 64)
    y_table = np.zeros((8, 4, 32, 2, 4, 64))
    for x in range(4):
        y_table[:, x, :, :, x, :] = both
    y_table = y_table.reshape(1024, 512).astype(ml_dtypes.bfloat16)
    r16 = np.arange(16)
    x_of = (16 * np.arange(16)[:, None] + (2 * (r16 % 8) + r16 // 8)[None, :]).reshape(256)
    cos_x, sin_x = waves(signed, x_of)
    x_table = np.concatenate(split_bf16(np.concatenate([cos_x, sin_x], axis=0)), axis=0)
    cos_x, sin_x = waves(signed, grid)
    xi_table = np.concatenate(split_bf16(np.concatenate([cos_x.T, sin_x.T], axis=0)), axis=1)
    c = cos_y.reshape(64, 8, 32)
    s = sin_y.reshape(64, 8, 32)
    yi_table = np.zeros((4, 2, 64, 2, 8, 4, 32))
    for x in range(4):
        yi_table[x, 0, :, 0, :, x, :] = c
        yi_table[x, 1, :, 0, :, x, :] = -s
        yi_table[x, 0, :, 1, :, x, :] = s
        yi_table[x, 1, :, 1, :, x, :] = c
    yi_table = yi_table.reshape(512, 2048).astype(ml_dtypes.bfloat16)
    factor = np.where(np.arange(32) == 0, 1.0, 2.0)[:, None] / 16777216.0
    back = np.stack([(factor * cos_z).reshape(8, 4, 256), (-factor * sin_z).reshape(8, 4, 256)], axis=1)
    zi = np.zeros((8, 2, 2, 4, 2, 256))
    for o in range(2):
        zi[:, :, o, :, o, :] = back
    zi_table = np.concatenate(split_bf16(zi.reshape(128, 512)), axis=0)
    return z_table, y_table, x_table, xi_table, yi_table, zi_table


def dot(a, b):
    return jnp.dot(a, b, preferred_element_type=F32)


def z_group(field_ref, table_ref, out_ref, group):
    for c in range(4):
        rows = field_ref[group * 4 + c].reshape(512, 256)
        both = lax.dot_general(
            table_ref[...], rows, (((1,), (1,)), ((), ())), preferred_element_type=F32
        )
        out_ref[:, group * 4 + c] = (both[:64] + both[64:]).reshape(8, 8, 512).astype(BF16)


def y_group(in_ref, table_ref, out_ref, rows_ref, group):
    part = pl.ds(group * 4, 4)
    left = jnp.concatenate(
        [
            jnp.concatenate(
                [in_ref[p, part, :, quad * 128 : (quad + 1) * 128].reshape(32, 128) for p in range(8)],
                axis=1,
            )
            for quad in range(4)
        ],
        axis=0,
    )
    both = dot(left, table_ref[...])
    turned = pltpu.roll(both[:, 256:].reshape(16, 8, 256), 4, 1)
    lower = lax.broadcasted_iota(jnp.int32, (16, 8, 256), 1) < 4
    value = both[:, :256].reshape(16, 8, 256) + jnp.where(lower, turned, -turned)
    value = value.reshape(128, 256)
    for quad in range(4):
        rows_ref[pl.ds(2 * quad, 32, stride=8), :] = value[quad * 32 : (quad + 1) * 32, :128]
        rows_ref[pl.ds(2 * quad + 1, 32, stride=8), :] = value[quad * 32 : (quad + 1) * 32, 128:]
    rows = rows_ref[...].reshape(4, 2, 4, 8, 128)
    real = rows[:, 0].reshape(128, 128)
    imag = rows[:, 1].reshape(128, 128)
    first = lax.broadcasted_iota(jnp.int32, (128, 128), 1) < 64
    even = jnp.where(first, real, pltpu.roll(imag, 64, 1)).reshape(4, 4, 8, 128)
    odd = jnp.where(first, pltpu.roll(real, 64, 1), imag).reshape(4, 4, 8, 128)
    out_ref[group] = jnp.concatenate([even, odd], axis=2).astype(BF16).reshape(16, 16, 128)


def x_group(in_ref, table_ref, out_ref, group, row, col):
    both = dot(table_ref[...], in_ref[group].reshape(256, 128))
    both = both[:128] + both[128:]
    turned = pltpu.roll(both[64:], 64, 1)
    first = lax.broadcasted_iota(jnp.int32, (64, 128), 1) < 64
    out_ref[group, row, col] = (both[:64] + jnp.where(first, turned, -turned)).astype(BF16)


def mix_group(spec_ref, weight_ref, sum_ref, group):
    for l in range(4):
        sums = [None] * 4
        for ci in range(4):
            c = 4 * group + ci
            value = spec_ref[group, ci, l].astype(F32)
            real = value[:, :64]
            imag = pltpu.roll(value, 64, 1)[:, :64]
            for o in range(2):
                wr = weight_ref[0, c, o, l].astype(F32)
                wi = weight_ref[1, c, o, l].astype(F32)
                for n, term in enumerate((real * wr - imag * wi, real * wi + imag * wr)):
                    sums[2 * o + n] = term if ci == 0 else sums[2 * o + n] + term
        for o in range(2):
            for n in range(2):
                sum_ref[o, l, n] += sums[2 * o + n]


def x_inverse(sum_ref, table_ref, out_ref, rows_ref):
    first = lax.broadcasted_iota(jnp.int32, (256, 128), 1) < 64
    for o in range(2):
        for l in range(4):
            mixed = jnp.concatenate([sum_ref[o, l, 0], sum_ref[o, l, 1]], axis=1).astype(BF16)
            both = dot(table_ref[...], jnp.concatenate([mixed, mixed], axis=0))
            turned = pltpu.roll(both[256:], 64, 1)
            rows_ref[pl.ds(o * 4 + l, 256, stride=8), :] = both[:256] + jnp.where(first, -turned, turned)
    out_ref[...] = rows_ref[...].astype(BF16).reshape(out_ref.shape)


def y_inverse(in_ref, table_ref, out_ref, group):
    part = pl.ds(group * 4, 4)
    left = jnp.concatenate(
        [
            jnp.concatenate(
                [in_ref[part, (quad * 4 + x) * 8 : (quad * 4 + x + 1) * 8, :].reshape(32, 128) for x in range(4)],
                axis=1,
            )
            for quad in range(4)
        ],
        axis=0,
    )
    for ri in range(2):
        value = dot(left, table_ref[:, ri * 1024 : (ri + 1) * 1024]).reshape(4, 4, 8, 1024).astype(BF16)
        for q in range(8):
            for quad in range(4):
                out_ref[q, part, ri, :, quad * 128 : (quad + 1) * 128] = value[quad, :, :, q * 128 : (q + 1) * 128]


def spread_point(point, spread):
    r = lax.broadcasted_iota(jnp.int32, (256, 32), 0)
    c = lax.broadcasted_iota(jnp.int32, (256, 32), 1)
    tall = ((r >= 8 * c) & (r < 8 * c + 8)).astype(F32).astype(BF16)
    r = lax.broadcasted_iota(jnp.int32, (32, 256), 0)
    c = lax.broadcasted_iota(jnp.int32, (32, 256), 1)
    wide = ((c >= 8 * r) & (c < 8 * r + 8)).astype(F32).astype(BF16)
    r = lax.broadcasted_iota(jnp.int32, (256, 256), 0)
    c = lax.broadcasted_iota(jnp.int32, (256, 256), 1)
    every = dot(dot(tall, point[...]).astype(BF16), wide)
    spread[...] = jnp.where((r & 7) == (c & 7), every, 0.0).astype(BF16)


def point_plane(field_ref, spread, out_ref, x):
    for y in range(4):
        rows = field_ref[:, x, y * 8 : (y + 1) * 8, :].reshape(256, 256)
        out_ref[:, x, y * 8 : (y + 1) * 8, :] = dot(spread[...], rows).reshape(32, 8, 256)


def activate(g, point_rows, bias, table_ref):
    value = lax.dot_general(
        jnp.concatenate([g, g], axis=0), table_ref[...], (((0,), (0,)), ((), ())), preferred_element_type=F32
    )
    out = []
    for o in range(2):
        total = value[:, o * 256 : (o + 1) * 256].reshape(4, 32, 256) + point_rows[o]
        total = total + bias[o]
        out.append((0.5 * total * (1.0 + lax.erf(total * 0.7071067811865476))).astype(BF16))
    return out


def transform(
    field_hbm, weight_hbm, zt_hbm, yt_hbm, xt_hbm, xit_hbm, yit_hbm, zit_hbm, point_hbm, bias_hbm,
    out_hbm, late_hbm, plane_hbm,
    field, weight, zt, yt, xt, xit, yit, zit, point, bias,
    z_out, y_in, y_rows, y_out, x_in, spec, sums, m_rows, m_out, b_in, b_out,
    spread, planes, f_in, stage,
    load_sem, field_sem, s1, r1, s2, r2, s3, r3, s4, r4, s5, r5, own_sem, out_sem,
):
    px = lax.axis_index("px")
    py = lax.axis_index("py")
    row = px // 4
    col = lax.rem(px, 4)

    def wrap(value, size):
        return lax.rem(value + size, size)

    def load_field(step):
        part = pl.ds(step * 4, 4)
        return pltpu.make_async_copy(field_hbm.at[part], field.at[part], field_sem.at[step])

    loads = [
        pltpu.make_async_copy(a, b, load_sem.at[n])
        for n, (a, b) in enumerate(
            ((zt_hbm, zt), (yt_hbm, yt), (xt_hbm, xt), (weight_hbm, weight), (xit_hbm, xit), (yit_hbm, yit),
             (zit_hbm, zit), (point_hbm, point), (bias_hbm, bias))
        )
    ]
    loads[0].start()
    for step in range(8):
        load_field(step).start()
    for load in loads[1:]:
        load.start()

    barrier = pltpu.get_barrier_semaphore()
    for d in range(1, 8):
        pl.semaphore_signal(barrier, inc=1, device_id={"py": wrap(py + d, 8)}, device_id_type=MESH)
    for d in range(1, 16):
        pl.semaphore_signal(barrier, inc=1, device_id={"px": wrap(px + d, 16)}, device_id_type=MESH)

    def remote(src, dst, send, recv, axis, peer):
        return pltpu.make_async_remote_copy(
            src_ref=src, dst_ref=dst, send_sem=send, recv_sem=recv, device_id={axis: peer}, device_id_type=MESH
        )

    def wait(view, semaphore):
        pltpu.make_async_copy(view, view, semaphore).wait()

    def send1(step, d, slot):
        part = pl.ds(step * 4, 4)
        peer = wrap(py + d, 8)
        return remote(z_out.at[peer, part], y_in.at[slot, part], s1, r1.at[step], "py", peer)

    def do_z(step):
        load_field(step).wait()
        z_group(field, zt, z_out, step)
        y_in[py, pl.ds(step * 4, 4)] = z_out[py, pl.ds(step * 4, 4)]

    def send_z(step):
        for d in range(1, 8):
            send1(step, d, py).start()

    loads[0].wait()
    do_z(0)
    pl.semaphore_wait(barrier, 22)
    send_z(0)

    def z_step(step, carry):
        do_z(step)
        send_z(step)
        return carry

    lax.fori_loop(1, 8, z_step, 0)

    def send2(step, peer, slot):
        return remote(y_out.at[step, peer], x_in.at[step, slot], s2, r2.at[step], "px", peer)

    def do_y(step):
        wait(y_in.at[pl.ds(0, 7), pl.ds(step * 4, 4)], r1.at[step])
        y_group(y_in, yt, y_out, y_rows, step)
        for d in range(1, 16):
            send2(step, wrap(px + d, 16), px).start()
        x_in[step, px] = y_out[step, px]

    halves = (pl.ds(0, 32), pl.ds(32, 32))

    def gather(step, phase, h, d):
        along_col = (h == 0) == (phase == 0)
        if phase == 0:
            place = spec.at[step, row, col, halves[h]]
        elif along_col:
            place = spec.at[step, :, col, halves[h]]
        else:
            place = spec.at[step, row, :, halves[h]]
        peer = 4 * row + wrap(col + d, 4) if along_col else 4 * wrap(row + d, 4) + col
        return remote(place, place, s3, r3.at[step, phase], "px", peer)

    def do_x(step):
        wait(x_in.at[step, pl.ds(0, 15)], r2.at[step])
        x_group(x_in, xt, spec, step, row, col)
        for d in (1, 3, 2):
            for h in range(2):
                gather(step, 0, h, d).start()

    def do_second(step):
        wait(spec.at[step, 0, pl.ds(0, 3)], r3.at[step, 0])
        for h in range(2):
            for d in (1, 3, 2):
                gather(step, 1, h, d).start()

    def do_mix(step):
        wait(spec.at[step, pl.ds(0, 3)], r3.at[step, 1])
        mix_group(spec, weight, sums, step)

    loads[1].wait()
    loads[2].wait()
    loads[3].wait()
    sums[...] = jnp.zeros_like(sums)
    loads[7].wait()
    spread_point(point, spread)

    def y_step(step, carry):
        do_y(step)
        point_plane(field, spread, planes, 2 * step)
        point_plane(field, spread, planes, 2 * step + 1)
        pl.when(step >= 1)(lambda: do_x(step - 1))
        pl.when(step >= 2)(lambda: do_second(step - 2))
        pl.when(step >= 5)(lambda: do_mix(step - 5))
        return carry

    lax.fori_loop(0, 8, y_step, 0)
    do_mix(3)
    do_x(7)
    do_second(6)
    do_mix(4)
    do_mix(5)
    do_second(7)
    do_mix(6)
    do_mix(7)

    loads[4].wait()
    x_inverse(sums, xit, m_out, m_rows)

    def send4(peer, slot, d):
        return remote(m_out.at[peer], b_in.at[slot], s4, r4.at[d], "px", peer)

    rows_order = (0, 1, 3, 2)
    for dr in rows_order:
        for dc in range(4):
            if dr or dc:
                peer = 4 * wrap(row - dr, 4) + wrap(col - dc, 4)
                send4(peer, px, dr).start()
    b_in[px] = m_out[px]

    last = 2
    late = pl.ds(8 * wrap(row + last, 4), 8)
    spare = pltpu.make_async_copy(planes.at[late], plane_hbm, own_sem.at[0])
    spare.start()

    def send5(dr, d):
        part = pl.ds(4 * wrap(row + dr, 4), 4)
        peer = wrap(py + d, 8)
        place = late_hbm.at[py] if dr == last else f_in.at[py, part]
        return remote(b_out.at[peer, part], place, s5, r5.at[dr], "py", peer)

    loads[5].wait()
    for dr in rows_order:
        wait(b_in.at[pl.ds(0, 4 if dr else 3)], r4.at[dr])
        part = pl.ds(4 * wrap(row + dr, 4), 4)
        y_inverse(b_in, yit, b_out, wrap(row + dr, 4))
        for d in range(1, 8):
            send5(dr, d).start()
        if dr == last:
            own = pltpu.make_async_copy(b_out.at[py, part], late_hbm.at[py], own_sem.at[1])
            own.start()
        else:
            f_in[py, part] = b_out[py, part]

    loads[6].wait()
    loads[8].wait()
    stores = []
    for n, dr in enumerate(rows_order[:3]):
        group = wrap(row + dr, 4)
        wait(f_in.at[pl.ds(0, 7), pl.ds(0, 4)], r5.at[dr])

        def final(pair, carry, n=n, group=group):
            op = 4 * group + pair
            for quad in range(4):
                g = f_in[:, op, :, :, quad * 128 : (quad + 1) * 128].reshape(128, 128)
                part = slice(4 * quad, 4 * quad + 4)
                done = activate(
                    g, [planes[2 * op + o, part] for o in range(2)], [bias[2 * op + o] for o in range(2)], zit
                )
                for o in range(2):
                    stage[n, 2 * pair + o, part] = done[o]
            return carry

        lax.fori_loop(0, 4, final, 0, unroll=2)
        store = pltpu.make_async_copy(stage.at[n], out_hbm.at[pl.ds(8 * group, 8)], out_sem.at[n])
        store.start()
        stores.append(store)
    wait(late_hbm.at[pl.ds(0, 7)], r5.at[last])
    spare.wait()
    own.wait()
    for store in stores:
        store.wait()

    wait(z_out.at[pl.ds(0, 7)], s1)
    wait(y_out.at[:, pl.ds(0, 15)], s2)
    wait(spec.at[:, 0, pl.ds(0, 3)], s3)
    wait(spec.at[:, pl.ds(0, 3)], s3)
    wait(m_out.at[pl.ds(0, 15)], s4)
    wait(b_out.at[pl.ds(0, 7)], s5)


def finish(early_hbm, late_hbm, plane_hbm, bias, zit_hbm, out_hbm, late, planes, zit, stage, held, sems):
    row = lax.axis_index("px") // 4
    group = lax.rem(row + 2, 4)

    def load_plane(quad):
        part = pl.ds(4 * quad, 4)
        return pltpu.make_async_copy(plane_hbm.at[:, part], planes.at[:, part], sems.at[quad])

    def store(quad):
        part = pl.ds(4 * quad, 4)
        return pltpu.make_async_copy(stage.at[:, part], out_hbm.at[pl.ds(8 * group, 8), part], sems.at[4 + quad])

    def through(n, j, inward):
        part = pl.ds(8 * lax.rem(row + (0, 1, 3)[n], 4) + 4 * j, 4)
        if inward:
            return pltpu.make_async_copy(early_hbm.at[part], held.at[n, j], sems.at[10 + 2 * n + j])
        return pltpu.make_async_copy(held.at[n, j], out_hbm.at[part], sems.at[16 + 2 * n + j])

    chunks = [(n, j) for n in range(3) for j in range(2)]
    first = [
        pltpu.make_async_copy(zit_hbm, zit, sems.at[8]),
        pltpu.make_async_copy(late_hbm, late, sems.at[9]),
    ]
    for copy in first:
        copy.start()
    for quad in range(4):
        load_plane(quad).start()
        if quad == 0:
            for n, j in chunks:
                through(n, j, True).start()
    for copy in first:
        copy.wait()
    for quad in range(4):
        load_plane(quad).wait()
        part = slice(4 * quad, 4 * quad + 4)
        for pair in range(4):
            g = late[:, pair, :, :, quad * 128 : (quad + 1) * 128].reshape(128, 128)
            done = activate(
                g,
                [planes[2 * pair + o, part] for o in range(2)],
                [bias[8 * group + 2 * pair + o] for o in range(2)],
                zit,
            )
            for o in range(2):
                stage[2 * pair + o, part] = done[o]
        store(quad).start()
        for n, j in chunks[2 * quad : 2 * quad + 2]:
            through(n, j, True).wait()
            through(n, j, False).start()
    for quad in range(4):
        store(quad).wait()
    for n, j in chunks:
        through(n, j, False).wait()


def body(tables, field, spectral_weight, point_weight, point_bias):
    z_table, y_table, x_table, xi_table, yi_table, zi_table = tables
    field = field.reshape(32, 16, 32, 256)
    anywhere = pl.BlockSpec(memory_space=pl.ANY)
    dma = pltpu.SemaphoreType.DMA
    operands = (field, spectral_weight, z_table, y_table, x_table, xi_table, yi_table, zi_table, point_weight)
    early, late, planes = pl.pallas_call(
        transform,
        out_shape=(
            jax.ShapeDtypeStruct((32, 16, 32, 256), BF16),
            jax.ShapeDtypeStruct((8, 4, 2, 8, 512), BF16),
            jax.ShapeDtypeStruct((8, 16, 32, 256), F32),
        ),
        in_specs=[anywhere] * (len(operands) + 1),
        out_specs=(anywhere,) * 3,
        scratch_shapes=[
            *[pltpu.VMEM(a.shape, a.dtype) for a in operands],
            pltpu.SMEM((32,), F32),
            pltpu.VMEM((8, 32, 8, 512), BF16),
            pltpu.VMEM((8, 32, 8, 512), BF16),
            pltpu.VMEM((256, 128), F32),
            pltpu.VMEM((8, 16, 16, 128), BF16),
            pltpu.VMEM((8, 16, 16, 128), BF16),
            pltpu.VMEM((8, 4, 4, 64, 128), BF16),
            pltpu.VMEM((2, 4, 2, 64, 64), F32),
            pltpu.VMEM((2048, 128), F32),
            pltpu.VMEM((16, 128, 128), BF16),
            pltpu.VMEM((16, 128, 128), BF16),
            pltpu.VMEM((8, 16, 2, 8, 512), BF16),
            pltpu.VMEM((256, 256), BF16),
            pltpu.VMEM((32, 16, 32, 256), F32),
            pltpu.VMEM((8, 16, 2, 8, 512), BF16),
            pltpu.VMEM((3, 8, 16, 32, 256), BF16),
            dma((9,)), dma((8,)),
            dma, dma((8,)),
            dma, dma((8,)),
            dma, dma((8, 2)),
            dma, dma((4,)),
            dma, dma((4,)),
            dma((2,)), dma((3,)),
        ],
        compiler_params=pltpu.CompilerParams(
            collective_id=1, has_side_effects=True, vmem_limit_bytes=VMEM_LIMIT
        ),
        name="transform",
    )(*operands, point_bias)
    out = pl.pallas_call(
        finish,
        out_shape=jax.ShapeDtypeStruct((32, 16, 32, 256), BF16),
        in_specs=[anywhere] * 3 + [pl.BlockSpec(memory_space=pltpu.SMEM), anywhere],
        out_specs=anywhere,
        scratch_shapes=[
            pltpu.VMEM((8, 4, 2, 8, 512), BF16),
            pltpu.VMEM((8, 16, 32, 256), F32),
            pltpu.VMEM((256, 512), BF16),
            pltpu.VMEM((8, 16, 32, 256), BF16),
            pltpu.VMEM((3, 2, 4, 16, 32, 256), BF16),
            dma((22,)),
        ],
        compiler_params=pltpu.CompilerParams(vmem_limit_bytes=VMEM_LIMIT),
        name="finish",
    )(early, late, planes, point_bias, zi_table)
    return out.reshape(1, 32, 16, 32, 256)


def solution(mesh):
    tables = tuple(jnp.asarray(t) for t in build_tables())

    def run(field, spectral_weight, point_weight, point_bias):
        return jax.shard_map(
            body,
            mesh=mesh,
            in_specs=((P(),) * 6, P(None, None, "px", "py", None), P(None, None, "px", "py", None, None), P(), P()),
            out_specs=P(None, None, "px", "py", None),
            check_vma=False,
        )(tables, field, spectral_weight, point_weight, point_bias)

    return run
```

```python
import functools

import jax
import jax.numpy as jnp
import ml_dtypes
import numpy as np
from jax import lax
from jax.experimental import pallas as pl
from jax.experimental.pallas import tpu as pltpu
from jax.sharding import PartitionSpec as P

F32 = jnp.float32
BF16 = jnp.bfloat16
MESH = pl.DeviceIdType.MESH
VMEM_LIMIT = 62 * 1024 * 1024


def split_bf16(table):
    high = table.astype(ml_dtypes.bfloat16)
    low = (table - high.astype(np.float64)).astype(ml_dtypes.bfloat16)
    return high, low


def waves(numbers, positions):
    turns = (np.outer(numbers, positions) % 256).astype(np.float64)
    angle = 2.0 * np.pi * turns / 256.0
    return np.cos(angle), np.sin(angle)


def build_tables():
    signed = np.concatenate([np.arange(32), np.arange(32) - 32])
    grid = np.arange(256)
    cos_z, sin_z = waves(np.arange(32), grid)
    z_rows = np.stack([cos_z.reshape(8, 4, 256), -sin_z.reshape(8, 4, 256)], axis=1).reshape(64, 256)
    z_table = np.concatenate(split_bf16(z_rows), axis=0)
    cos_y, sin_y = waves(signed, grid)
    both = np.stack([cos_y, sin_y], axis=0).transpose(2, 0, 1).reshape(8, 32, 2, 64)
    y_table = np.zeros((8, 4, 32, 2, 4, 64))
    for x in range(4):
        y_table[:, x, :, :, x, :] = both
    y_table = y_table.reshape(1024, 512).astype(ml_dtypes.bfloat16)
    r16 = np.arange(16)
    x_of = (16 * np.arange(16)[:, None] + (2 * (r16 % 8) + r16 // 8)[None, :]).reshape(256)
    cos_x, sin_x = waves(signed, x_of)
    x_table = np.concatenate(split_bf16(np.concatenate([cos_x, sin_x], axis=0)), axis=0)
    cos_x, sin_x = waves(signed, grid)
    xi_table = np.concatenate(split_bf16(np.concatenate([cos_x.T, sin_x.T], axis=0)), axis=1)
    c = cos_y.reshape(64, 8, 32)
    s = sin_y.reshape(64, 8, 32)
    yi_table = np.zeros((4, 2, 64, 2, 8, 4, 32))
    for x in range(4):
        yi_table[x, 0, :, 0, :, x, :] = c
        yi_table[x, 1, :, 0, :, x, :] = -s
        yi_table[x, 0, :, 1, :, x, :] = s
        yi_table[x, 1, :, 1, :, x, :] = c
    yi_table = yi_table.reshape(512, 2048).astype(ml_dtypes.bfloat16)
    factor = np.where(np.arange(32) == 0, 1.0, 2.0)[:, None] / 16777216.0
    back = np.stack([(factor * cos_z).reshape(8, 4, 256), (-factor * sin_z).reshape(8, 4, 256)], axis=1)
    zi = np.zeros((8, 2, 2, 4, 2, 256))
    for o in range(2):
        zi[:, :, o, :, o, :] = back
    zi_table = np.concatenate(split_bf16(zi.reshape(128, 512)), axis=0)
    return z_table, y_table, x_table, xi_table, yi_table, zi_table


def dot(a, b):
    return jnp.dot(a, b, preferred_element_type=F32)


def z_group(field_ref, table_ref, out_ref, group):
    for c in range(4):
        rows = field_ref[group * 4 + c].reshape(512, 256)
        both = lax.dot_general(
            table_ref[...], rows, (((1,), (1,)), ((), ())), preferred_element_type=F32
        )
        out_ref[:, group * 4 + c] = (both[:64] + both[64:]).reshape(8, 8, 512).astype(BF16)


def y_group(in_ref, table_ref, out_ref, rows_ref, group):
    part = pl.ds(group * 4, 4)
    left = jnp.concatenate(
        [
            jnp.concatenate(
                [in_ref[p, part, :, quad * 128 : (quad + 1) * 128].reshape(32, 128) for p in range(8)],
                axis=1,
            )
            for quad in range(4)
        ],
        axis=0,
    )
    both = dot(left, table_ref[...])
    turned = pltpu.roll(both[:, 256:].reshape(16, 8, 256), 4, 1)
    lower = lax.broadcasted_iota(jnp.int32, (16, 8, 256), 1) < 4
    value = both[:, :256].reshape(16, 8, 256) + jnp.where(lower, turned, -turned)
    value = value.reshape(128, 256)
    for quad in range(4):
        rows_ref[pl.ds(2 * quad, 32, stride=8), :] = value[quad * 32 : (quad + 1) * 32, :128]
        rows_ref[pl.ds(2 * quad + 1, 32, stride=8), :] = value[quad * 32 : (quad + 1) * 32, 128:]
    rows = rows_ref[...].reshape(4, 2, 4, 8, 128)
    real = rows[:, 0].reshape(128, 128)
    imag = rows[:, 1].reshape(128, 128)
    first = lax.broadcasted_iota(jnp.int32, (128, 128), 1) < 64
    even = jnp.where(first, real, pltpu.roll(imag, 64, 1)).reshape(4, 4, 8, 128)
    odd = jnp.where(first, pltpu.roll(real, 64, 1), imag).reshape(4, 4, 8, 128)
    out_ref[group] = jnp.concatenate([even, odd], axis=2).astype(BF16).reshape(16, 16, 128)


def x_group(in_ref, table_ref, out_ref, group, row, col):
    both = dot(table_ref[...], in_ref[group].reshape(256, 128))
    both = both[:128] + both[128:]
    turned = pltpu.roll(both[64:], 64, 1)
    first = lax.broadcasted_iota(jnp.int32, (64, 128), 1) < 64
    out_ref[group, row, col] = (both[:64] + jnp.where(first, turned, -turned)).astype(BF16)


def mix_group(spec_ref, weight_ref, sum_ref, group):
    for l in range(4):
        sums = [None] * 4
        for ci in range(4):
            c = 4 * group + ci
            value = spec_ref[group, ci, l].astype(F32)
            real = value[:, :64]
            imag = pltpu.roll(value, 64, 1)[:, :64]
            for o in range(2):
                wr = weight_ref[0, c, o, l].astype(F32)
                wi = weight_ref[1, c, o, l].astype(F32)
                for n, term in enumerate((real * wr - imag * wi, real * wi + imag * wr)):
                    sums[2 * o + n] = term if ci == 0 else sums[2 * o + n] + term
        for o in range(2):
            for n in range(2):
                sum_ref[o, l, n] += sums[2 * o + n]


def x_inverse(sum_ref, table_ref, out_ref, rows_ref):
    first = lax.broadcasted_iota(jnp.int32, (256, 128), 1) < 64
    for o in range(2):
        for l in range(4):
            mixed = jnp.concatenate([sum_ref[o, l, 0], sum_ref[o, l, 1]], axis=1).astype(BF16)
            both = dot(table_ref[...], jnp.concatenate([mixed, mixed], axis=0))
            turned = pltpu.roll(both[256:], 64, 1)
            rows_ref[pl.ds(o * 4 + l, 256, stride=8), :] = both[:256] + jnp.where(first, -turned, turned)
    out_ref[...] = rows_ref[...].astype(BF16).reshape(out_ref.shape)


def y_inverse(in_ref, table_ref, out_ref, group):
    part = pl.ds(group * 4, 4)
    left = jnp.concatenate(
        [
            jnp.concatenate(
                [in_ref[part, (quad * 4 + x) * 8 : (quad * 4 + x + 1) * 8, :].reshape(32, 128) for x in range(4)],
                axis=1,
            )
            for quad in range(4)
        ],
        axis=0,
    )
    for ri in range(2):
        value = dot(left, table_ref[:, ri * 1024 : (ri + 1) * 1024]).reshape(4, 4, 8, 1024).astype(BF16)
        for q in range(8):
            for quad in range(4):
                out_ref[q, part, ri, :, quad * 128 : (quad + 1) * 128] = value[quad, :, :, q * 128 : (q + 1) * 128]


def spread_point(point, spread):
    r = lax.broadcasted_iota(jnp.int32, (256, 32), 0)
    c = lax.broadcasted_iota(jnp.int32, (256, 32), 1)
    tall = ((r >= 8 * c) & (r < 8 * c + 8)).astype(F32).astype(BF16)
    r = lax.broadcasted_iota(jnp.int32, (32, 256), 0)
    c = lax.broadcasted_iota(jnp.int32, (32, 256), 1)
    wide = ((c >= 8 * r) & (c < 8 * r + 8)).astype(F32).astype(BF16)
    r = lax.broadcasted_iota(jnp.int32, (256, 256), 0)
    c = lax.broadcasted_iota(jnp.int32, (256, 256), 1)
    every = dot(dot(tall, point[...]).astype(BF16), wide)
    spread[...] = jnp.where((r & 7) == (c & 7), every, 0.0).astype(BF16)


def point_plane(field_ref, spread, out_ref, x):
    for y in range(4):
        rows = field_ref[:, x, y * 8 : (y + 1) * 8, :].reshape(256, 256)
        out_ref[:, x, y * 8 : (y + 1) * 8, :] = dot(spread[...], rows).reshape(32, 8, 256)


def activate(g, point_rows, bias, table_ref):
    value = lax.dot_general(
        jnp.concatenate([g, g], axis=0), table_ref[...], (((0,), (0,)), ((), ())), preferred_element_type=F32
    )
    out = []
    for o in range(2):
        total = value[:, o * 256 : (o + 1) * 256].reshape(4, 32, 256) + point_rows[o]
        total = total + bias[o]
        out.append((0.5 * total * (1.0 + lax.erf(total * 0.7071067811865476))).astype(BF16))
    return out


def transform(
    field_hbm, weight_hbm, zt_hbm, yt_hbm, xt_hbm, xit_hbm, yit_hbm, zit_hbm, point_hbm, bias_hbm,
    out_hbm, late_hbm, plane_hbm,
    field, weight, zt, yt, xt, xit, yit, zit, point, bias,
    z_out, y_in, y_rows, y_out, x_in, spec, sums, m_rows, m_out, b_in, b_out,
    spread, planes, narrow, f_in, stage,
    load_sem, field_sem, s1, r1, s2, r2, s3, r3, s4, r4, s5, r5, own_sem, out_sem, r6,
):
    px = lax.axis_index("px")
    py = lax.axis_index("py")
    row = px // 4
    col = lax.rem(px, 4)

    def wrap(value, size):
        return lax.rem(value + size, size)

    def load_field(step):
        part = pl.ds(step * 4, 4)
        return pltpu.make_async_copy(field_hbm.at[part], field.at[part], field_sem.at[step])

    loads = [
        pltpu.make_async_copy(a, b, load_sem.at[n])
        for n, (a, b) in enumerate(
            ((zt_hbm, zt), (yt_hbm, yt), (xt_hbm, xt), (weight_hbm, weight), (xit_hbm, xit), (yit_hbm, yit),
             (zit_hbm, zit), (point_hbm, point), (bias_hbm, bias))
        )
    ]
    loads[0].start()
    for step in range(8):
        load_field(step).start()
    for load in loads[1:]:
        load.start()

    barrier = pltpu.get_barrier_semaphore()
    for d in range(1, 8):
        pl.semaphore_signal(barrier, inc=1, device_id={"py": wrap(py + d, 8)}, device_id_type=MESH)
    for d in range(1, 16):
        pl.semaphore_signal(barrier, inc=1, device_id={"px": wrap(px + d, 16)}, device_id_type=MESH)

    def remote(src, dst, send, recv, axis, peer):
        return pltpu.make_async_remote_copy(
            src_ref=src, dst_ref=dst, send_sem=send, recv_sem=recv, device_id={axis: peer}, device_id_type=MESH
        )

    def wait(view, semaphore):
        pltpu.make_async_copy(view, view, semaphore).wait()

    def send1(step, d, slot):
        part = pl.ds(step * 4, 4)
        peer = wrap(py + d, 8)
        return remote(z_out.at[peer, part], y_in.at[slot, part], s1, r1.at[step], "py", peer)

    def do_z(step):
        load_field(step).wait()
        z_group(field, zt, z_out, step)
        y_in[py, pl.ds(step * 4, 4)] = z_out[py, pl.ds(step * 4, 4)]

    def send_z(step):
        for d in range(1, 8):
            send1(step, d, py).start()

    loads[0].wait()
    do_z(0)
    pl.semaphore_wait(barrier, 22)
    send_z(0)

    def z_step(step, carry):
        do_z(step)
        send_z(step)
        return carry

    lax.fori_loop(1, 8, z_step, 0)

    def send2(step, peer, slot):
        return remote(y_out.at[step, peer], x_in.at[step, slot], s2, r2.at[step], "px", peer)

    def do_y(step):
        wait(y_in.at[pl.ds(0, 7), pl.ds(step * 4, 4)], r1.at[step])
        y_group(y_in, yt, y_out, y_rows, step)
        for d in range(1, 16):
            send2(step, wrap(px + d, 16), px).start()
        x_in[step, px] = y_out[step, px]

    halves = (pl.ds(0, 32), pl.ds(32, 32))

    def gather(step, phase, h, d):
        along_col = (h == 0) == (phase == 0)
        if phase == 0:
            place = spec.at[step, row, col, halves[h]]
        elif along_col:
            place = spec.at[step, :, col, halves[h]]
        else:
            place = spec.at[step, row, :, halves[h]]
        peer = 4 * row + wrap(col + d, 4) if along_col else 4 * wrap(row + d, 4) + col
        return remote(place, place, s3, r3.at[step, phase], "px", peer)

    def do_x(step, direct=False):
        wait(x_in.at[step, pl.ds(0, 15)], r2.at[step])
        x_group(x_in, xt, spec, step, row, col)
        if direct:
            place = spec.at[step, row, col]
            for d in range(1, 16):
                remote(place, place, s3, r6, "px", wrap(px + d, 16)).start()
            return
        for d in (1, 3, 2):
            for h in range(2):
                gather(step, 0, h, d).start()

    def do_second(step):
        wait(spec.at[step, 0, pl.ds(0, 3)], r3.at[step, 0])
        for h in range(2):
            for d in (1, 3, 2):
                gather(step, 1, h, d).start()

    def do_mix(step, direct=False):
        if direct:
            wait(spec.at[pl.ds(0, 5), pl.ds(0, 3), 0], r6)
        else:
            wait(spec.at[step, pl.ds(0, 3)], r3.at[step, 1])
        mix_group(spec, weight, sums, step)

    loads[1].wait()
    loads[2].wait()
    loads[3].wait()
    sums[...] = jnp.zeros_like(sums)
    loads[7].wait()
    spread_point(point, spread)

    def y_step(step, carry):
        do_y(step)
        point_plane(field, spread, planes, 2 * step)
        point_plane(field, spread, planes, 2 * step + 1)
        pl.when(step >= 2)(lambda: do_x(step - 2))
        pl.when(step >= 3)(lambda: do_second(step - 3))
        pl.when(step >= 6)(lambda: do_mix(step - 6))
        return carry

    lax.fori_loop(0, 8, y_step, 0)
    do_x(6)
    do_second(5)
    do_mix(2)
    do_x(7, True)
    do_second(6)
    do_mix(3)
    do_mix(4)
    do_mix(5)
    do_mix(6)
    do_mix(7, True)

    loads[4].wait()
    x_inverse(sums, xit, m_out, m_rows)

    def send4(peer, slot, d):
        return remote(m_out.at[peer], b_in.at[slot], s4, r4.at[d], "px", peer)

    rows_order = (0, 1, 3, 2)
    for dr in rows_order:
        for dc in range(4):
            if dr or dc:
                peer = 4 * wrap(row - dr, 4) + wrap(col - dc, 4)
                send4(peer, px, dr).start()
    b_in[px] = m_out[px]

    last = 2
    late = pl.ds(8 * wrap(row + last, 4), 8)
    narrow[...] = planes[late].astype(BF16)
    spare = pltpu.make_async_copy(narrow, plane_hbm, own_sem.at[0])
    spare.start()

    def send5(dr, d):
        part = pl.ds(4 * wrap(row + dr, 4), 4)
        peer = wrap(py + d, 8)
        place = late_hbm.at[py] if dr == last else f_in.at[py, part]
        return remote(b_out.at[peer, part], place, s5, r5.at[dr], "py", peer)

    loads[5].wait()
    for dr in rows_order:
        wait(b_in.at[pl.ds(0, 4 if dr else 3)], r4.at[dr])
        part = pl.ds(4 * wrap(row + dr, 4), 4)
        y_inverse(b_in, yit, b_out, wrap(row + dr, 4))
        for d in range(1, 8):
            send5(dr, d).start()
        if dr == last:
            own = pltpu.make_async_copy(b_out.at[py, part], late_hbm.at[py], own_sem.at[1])
            own.start()
        else:
            f_in[py, part] = b_out[py, part]

    loads[6].wait()
    loads[8].wait()
    stores = []
    for n, dr in enumerate(rows_order[:3]):
        group = wrap(row + dr, 4)
        wait(f_in.at[pl.ds(0, 7), pl.ds(0, 4)], r5.at[dr])

        def final(pair, carry, n=n, group=group):
            op = 4 * group + pair
            for quad in range(4):
                g = f_in[:, op, :, :, quad * 128 : (quad + 1) * 128].reshape(128, 128)
                part = slice(4 * quad, 4 * quad + 4)
                done = activate(
                    g, [planes[2 * op + o, part] for o in range(2)], [bias[2 * op + o] for o in range(2)], zit
                )
                for o in range(2):
                    stage[n, 2 * pair + o, part] = done[o]
            return carry

        lax.fori_loop(0, 4, final, 0, unroll=2)
        store = pltpu.make_async_copy(stage.at[n], out_hbm.at[pl.ds(8 * group, 8)], out_sem.at[n])
        store.start()
        stores.append(store)
    wait(late_hbm.at[pl.ds(0, 7)], r5.at[last])
    spare.wait()
    own.wait()
    for store in stores:
        store.wait()

    wait(z_out.at[pl.ds(0, 7)], s1)
    wait(y_out.at[:, pl.ds(0, 15)], s2)
    wait(spec.at[:, 0, pl.ds(0, 3)], s3)
    wait(spec.at[:, pl.ds(0, 3)], s3)
    wait(m_out.at[pl.ds(0, 15)], s4)
    wait(b_out.at[pl.ds(0, 7)], s5)


def finish(early_hbm, late_hbm, plane_hbm, bias, zit_hbm, out_hbm, late, planes, zit, stage, held, sems):
    row = lax.axis_index("px") // 4
    group = lax.rem(row + 2, 4)

    def load_plane(quad):
        part = pl.ds(4 * quad, 4)
        return pltpu.make_async_copy(plane_hbm.at[:, part], planes.at[:, part], sems.at[quad])

    def store(quad):
        part = pl.ds(4 * quad, 4)
        return pltpu.make_async_copy(stage.at[:, part], out_hbm.at[pl.ds(8 * group, 8), part], sems.at[4 + quad])

    def through(n, j, inward):
        part = pl.ds(8 * lax.rem(row + (0, 1, 3)[n], 4) + 4 * j, 4)
        if inward:
            return pltpu.make_async_copy(early_hbm.at[part], held.at[n, j], sems.at[10 + 2 * n + j])
        return pltpu.make_async_copy(held.at[n, j], out_hbm.at[part], sems.at[16 + 2 * n + j])

    chunks = [(n, j) for n in range(3) for j in range(2)]
    first = [
        pltpu.make_async_copy(zit_hbm, zit, sems.at[8]),
        pltpu.make_async_copy(late_hbm, late, sems.at[9]),
    ]
    for copy in first:
        copy.start()
    for quad in range(4):
        load_plane(quad).start()
        if quad == 0:
            for n, j in chunks:
                through(n, j, True).start()
    for copy in first:
        copy.wait()
    for quad in range(4):
        load_plane(quad).wait()
        part = slice(4 * quad, 4 * quad + 4)
        for pair in range(4):
            g = late[:, pair, :, :, quad * 128 : (quad + 1) * 128].reshape(128, 128)
            done = activate(
                g,
                [planes[2 * pair + o, part].astype(F32) for o in range(2)],
                [bias[8 * group + 2 * pair + o] for o in range(2)],
                zit,
            )
            for o in range(2):
                stage[2 * pair + o, part] = done[o]
        store(quad).start()
        for n, j in chunks[2 * quad : 2 * quad + 2]:
            through(n, j, True).wait()
            through(n, j, False).start()
    for quad in range(4):
        store(quad).wait()
    for n, j in chunks:
        through(n, j, False).wait()


def body(tables, field, spectral_weight, point_weight, point_bias):
    z_table, y_table, x_table, xi_table, yi_table, zi_table = tables
    field = field.reshape(32, 16, 32, 256)
    anywhere = pl.BlockSpec(memory_space=pl.ANY)
    dma = pltpu.SemaphoreType.DMA
    operands = (field, spectral_weight, z_table, y_table, x_table, xi_table, yi_table, zi_table, point_weight)
    early, late, planes = pl.pallas_call(
        transform,
        out_shape=(
            jax.ShapeDtypeStruct((32, 16, 32, 256), BF16),
            jax.ShapeDtypeStruct((8, 4, 2, 8, 512), BF16),
            jax.ShapeDtypeStruct((8, 16, 32, 256), BF16),
        ),
        in_specs=[anywhere] * (len(operands) + 1),
        out_specs=(anywhere,) * 3,
        scratch_shapes=[
            *[pltpu.VMEM(a.shape, a.dtype) for a in operands],
            pltpu.SMEM((32,), F32),
            pltpu.VMEM((8, 32, 8, 512), BF16),
            pltpu.VMEM((8, 32, 8, 512), BF16),
            pltpu.VMEM((256, 128), F32),
            pltpu.VMEM((8, 16, 16, 128), BF16),
            pltpu.VMEM((8, 16, 16, 128), BF16),
            pltpu.VMEM((8, 4, 4, 64, 128), BF16),
            pltpu.VMEM((2, 4, 2, 64, 64), F32),
            pltpu.VMEM((2048, 128), F32),
            pltpu.VMEM((16, 128, 128), BF16),
            pltpu.VMEM((16, 128, 128), BF16),
            pltpu.VMEM((8, 16, 2, 8, 512), BF16),
            pltpu.VMEM((256, 256), BF16),
            pltpu.VMEM((32, 16, 32, 256), F32),
            pltpu.VMEM((8, 16, 32, 256), BF16),
            pltpu.VMEM((8, 16, 2, 8, 512), BF16),
            pltpu.VMEM((3, 8, 16, 32, 256), BF16),
            dma((9,)), dma((8,)),
            dma, dma((8,)),
            dma, dma((8,)),
            dma, dma((8, 2)),
            dma, dma((4,)),
            dma, dma((4,)),
            dma((2,)), dma((3,)), dma,
        ],
        compiler_params=pltpu.CompilerParams(
            collective_id=1, has_side_effects=True, vmem_limit_bytes=VMEM_LIMIT
        ),
        name="transform",
    )(*operands, point_bias)
    out = pl.pallas_call(
        finish,
        out_shape=jax.ShapeDtypeStruct((32, 16, 32, 256), BF16),
        in_specs=[anywhere] * 3 + [pl.BlockSpec(memory_space=pltpu.SMEM), anywhere],
        out_specs=anywhere,
        scratch_shapes=[
            pltpu.VMEM((8, 4, 2, 8, 512), BF16),
            pltpu.VMEM((8, 16, 32, 256), BF16),
            pltpu.VMEM((256, 512), BF16),
            pltpu.VMEM((8, 16, 32, 256), BF16),
            pltpu.VMEM((3, 2, 4, 16, 32, 256), BF16),
            dma((22,)),
        ],
        compiler_params=pltpu.CompilerParams(vmem_limit_bytes=VMEM_LIMIT),
        name="finish",
    )(early, late, planes, point_bias, zi_table)
    return out.reshape(1, 32, 16, 32, 256)


def solution(mesh):
    tables = tuple(jnp.asarray(t) for t in build_tables())

    def run(field, spectral_weight, point_weight, point_bias):
        return jax.shard_map(
            body,
            mesh=mesh,
            in_specs=((P(),) * 6, P(None, None, "px", "py", None), P(None, None, "px", "py", None, None), P(), P()),
            out_specs=P(None, None, "px", "py", None),
            check_vma=False,
        )(tables, field, spectral_weight, point_weight, point_bias)

    return run
```

```python
import functools

import jax
import jax.numpy as jnp
import ml_dtypes
import numpy as np
from jax import lax
from jax.experimental import pallas as pl
from jax.experimental.pallas import tpu as pltpu
from jax.sharding import PartitionSpec as P

F32 = jnp.float32
BF16 = jnp.bfloat16
MESH = pl.DeviceIdType.MESH
VMEM_LIMIT = 60 * 1024 * 1024


def split_bf16(table):
    high = table.astype(ml_dtypes.bfloat16)
    low = (table - high.astype(np.float64)).astype(ml_dtypes.bfloat16)
    return high, low


def waves(numbers, positions):
    turns = (np.outer(numbers, positions) % 256).astype(np.float64)
    angle = 2.0 * np.pi * turns / 256.0
    return np.cos(angle), np.sin(angle)


def build_tables():
    signed = np.concatenate([np.arange(32), np.arange(32) - 32])
    grid = np.arange(256)
    cos_z, sin_z = waves(np.arange(32), grid)
    z_rows = np.stack([cos_z.reshape(8, 4, 256), -sin_z.reshape(8, 4, 256)], axis=1).reshape(64, 256)
    z_table = np.concatenate(split_bf16(z_rows), axis=0)
    cos_y, sin_y = waves(signed, grid)
    both = np.stack([cos_y, sin_y], axis=0).transpose(2, 0, 1).reshape(8, 32, 2, 64)
    y_table = np.zeros((8, 4, 32, 2, 4, 64))
    for x in range(4):
        y_table[:, x, :, :, x, :] = both
    y_table = y_table.reshape(1024, 512).astype(ml_dtypes.bfloat16)
    r16 = np.arange(16)
    x_of = (16 * np.arange(16)[:, None] + (2 * (r16 % 8) + r16 // 8)[None, :]).reshape(256)
    cos_x, sin_x = waves(signed, x_of)
    x_table = np.concatenate(split_bf16(np.concatenate([cos_x, sin_x], axis=0)), axis=0)
    cos_x, sin_x = waves(signed, grid)
    xi_table = np.concatenate(split_bf16(np.concatenate([cos_x.T, sin_x.T], axis=0)), axis=1)
    c = cos_y.reshape(64, 8, 32)
    s = sin_y.reshape(64, 8, 32)
    yi_table = np.zeros((4, 2, 64, 2, 8, 4, 32))
    for x in range(4):
        yi_table[x, 0, :, 0, :, x, :] = c
        yi_table[x, 1, :, 0, :, x, :] = -s
        yi_table[x, 0, :, 1, :, x, :] = s
        yi_table[x, 1, :, 1, :, x, :] = c
    yi_table = yi_table.reshape(512, 2048).astype(ml_dtypes.bfloat16)
    factor = np.where(np.arange(32) == 0, 1.0, 2.0)[:, None] / 16777216.0
    back = np.stack([(factor * cos_z).reshape(8, 4, 256), (-factor * sin_z).reshape(8, 4, 256)], axis=1)
    zi = np.zeros((8, 2, 2, 4, 2, 256))
    for o in range(2):
        zi[:, :, o, :, o, :] = back
    zi_table = np.concatenate(split_bf16(zi.reshape(128, 512)), axis=0)
    return z_table, y_table, x_table, xi_table, yi_table, zi_table


def dot(a, b):
    return jnp.dot(a, b, preferred_element_type=F32)


def z_group(field_ref, table_ref, out_ref, group):
    for c in range(4):
        rows = field_ref[group * 4 + c].reshape(512, 256)
        both = lax.dot_general(
            table_ref[...], rows, (((1,), (1,)), ((), ())), preferred_element_type=F32
        )
        out_ref[:, group * 4 + c] = (both[:64] + both[64:]).reshape(8, 8, 512).astype(BF16)


def y_group(in_ref, table_ref, out_ref, rows_ref, group):
    part = pl.ds(group * 4, 4)
    left = jnp.concatenate(
        [
            jnp.concatenate(
                [in_ref[p, part, :, quad * 128 : (quad + 1) * 128].reshape(32, 128) for p in range(8)],
                axis=1,
            )
            for quad in range(4)
        ],
        axis=0,
    )
    both = dot(left, table_ref[...])
    turned = pltpu.roll(both[:, 256:].reshape(16, 8, 256), 4, 1)
    lower = lax.broadcasted_iota(jnp.int32, (16, 8, 256), 1) < 4
    value = both[:, :256].reshape(16, 8, 256) + jnp.where(lower, turned, -turned)
    value = value.reshape(128, 256)
    for quad in range(4):
        rows_ref[pl.ds(2 * quad, 32, stride=8), :] = value[quad * 32 : (quad + 1) * 32, :128]
        rows_ref[pl.ds(2 * quad + 1, 32, stride=8), :] = value[quad * 32 : (quad + 1) * 32, 128:]
    rows = rows_ref[...].reshape(4, 2, 4, 8, 128)
    real = rows[:, 0].reshape(128, 128)
    imag = rows[:, 1].reshape(128, 128)
    first = lax.broadcasted_iota(jnp.int32, (128, 128), 1) < 64
    even = jnp.where(first, real, pltpu.roll(imag, 64, 1)).reshape(4, 4, 8, 128)
    odd = jnp.where(first, pltpu.roll(real, 64, 1), imag).reshape(4, 4, 8, 128)
    out_ref[group] = jnp.concatenate([even, odd], axis=2).astype(BF16).reshape(16, 16, 128)


def x_group(in_ref, table_ref, out_ref, group, row, col):
    both = dot(table_ref[...], in_ref[group].reshape(256, 128))
    both = both[:128] + both[128:]
    turned = pltpu.roll(both[64:], 64, 1)
    first = lax.broadcasted_iota(jnp.int32, (64, 128), 1) < 64
    out_ref[group, row, col] = (both[:64] + jnp.where(first, turned, -turned)).astype(BF16)


def mix_group(spec_ref, weight_ref, sum_ref, group):
    for l in range(4):
        sums = [None] * 4
        for ci in range(4):
            c = 4 * group + ci
            value = spec_ref[group, ci, l].astype(F32)
            real = value[:, :64]
            imag = pltpu.roll(value, 64, 1)[:, :64]
            for o in range(2):
                wr = weight_ref[0, c, o, l].astype(F32)
                wi = weight_ref[1, c, o, l].astype(F32)
                for n, term in enumerate((real * wr - imag * wi, real * wi + imag * wr)):
                    sums[2 * o + n] = term if ci == 0 else sums[2 * o + n] + term
        for o in range(2):
            for n in range(2):
                sum_ref[o, l, n] += sums[2 * o + n]


def x_inverse(sum_ref, table_ref, out_ref, rows_ref):
    first = lax.broadcasted_iota(jnp.int32, (256, 128), 1) < 64
    for o in range(2):
        for l in range(4):
            mixed = jnp.concatenate([sum_ref[o, l, 0], sum_ref[o, l, 1]], axis=1).astype(BF16)
            both = dot(table_ref[...], jnp.concatenate([mixed, mixed], axis=0))
            turned = pltpu.roll(both[256:], 64, 1)
            rows_ref[pl.ds(o * 4 + l, 256, stride=8), :] = both[:256] + jnp.where(first, -turned, turned)
    out_ref[...] = rows_ref[...].astype(BF16).reshape(out_ref.shape)


def y_inverse(in_ref, table_ref, out_ref, group):
    part = pl.ds(group * 4, 4)
    left = jnp.concatenate(
        [
            jnp.concatenate(
                [in_ref[part, (quad * 4 + x) * 8 : (quad * 4 + x + 1) * 8, :].reshape(32, 128) for x in range(4)],
                axis=1,
            )
            for quad in range(4)
        ],
        axis=0,
    )
    for ri in range(2):
        value = dot(left, table_ref[:, ri * 1024 : (ri + 1) * 1024]).reshape(4, 4, 8, 1024).astype(BF16)
        for q in range(8):
            for quad in range(4):
                out_ref[q, part, ri, :, quad * 128 : (quad + 1) * 128] = value[quad, :, :, q * 128 : (q + 1) * 128]


def spread_point(point, spread):
    r = lax.broadcasted_iota(jnp.int32, (256, 32), 0)
    c = lax.broadcasted_iota(jnp.int32, (256, 32), 1)
    tall = ((r >= 8 * c) & (r < 8 * c + 8)).astype(F32).astype(BF16)
    r = lax.broadcasted_iota(jnp.int32, (32, 256), 0)
    c = lax.broadcasted_iota(jnp.int32, (32, 256), 1)
    wide = ((c >= 8 * r) & (c < 8 * r + 8)).astype(F32).astype(BF16)
    r = lax.broadcasted_iota(jnp.int32, (256, 256), 0)
    c = lax.broadcasted_iota(jnp.int32, (256, 256), 1)
    every = dot(dot(tall, point[...]).astype(BF16), wide)
    spread[...] = jnp.where((r & 7) == (c & 7), every, 0.0).astype(BF16)


def point_plane(field_ref, spread, out_ref, x):
    for y in range(4):
        rows = field_ref[:, x, y * 8 : (y + 1) * 8, :].reshape(256, 256)
        out_ref[:, x, y * 8 : (y + 1) * 8, :] = dot(spread[...], rows).reshape(32, 8, 256)


def activate(g, point_rows, bias, table_ref):
    value = lax.dot_general(
        jnp.concatenate([g, g], axis=0), table_ref[...], (((0,), (0,)), ((), ())), preferred_element_type=F32
    )
    out = []
    for o in range(2):
        total = value[:, o * 256 : (o + 1) * 256].reshape(4, 32, 256) + point_rows[o]
        total = total + bias[o]
        out.append((0.5 * total * (1.0 + lax.erf(total * 0.7071067811865476))).astype(BF16))
    return out


def transform(
    field_hbm, weight_hbm, zt_hbm, yt_hbm, xt_hbm, xit_hbm, yit_hbm, zit_hbm, point_hbm, bias_hbm,
    out_hbm, late_hbm, plane_hbm,
    field, weight, zt, yt, xt, xit, yit, zit, point, bias,
    z_out, y_in, y_rows, y_out, x_in, spec, sums, m_rows, m_out, b_in, b_out,
    spread, planes, f_in, stage,
    load_sem, field_sem, s1, r1, s2, r2, s3, r3, s4, r4, s5, r5, own_sem, out_sem,
):
    px = lax.axis_index("px")
    py = lax.axis_index("py")
    row = px // 4
    col = lax.rem(px, 4)

    def wrap(value, size):
        return lax.rem(value + size, size)

    def load_field(step):
        part = pl.ds(step * 4, 4)
        return pltpu.make_async_copy(field_hbm.at[part], field.at[part], field_sem.at[step])

    loads = [
        pltpu.make_async_copy(a, b, load_sem.at[n])
        for n, (a, b) in enumerate(
            ((zt_hbm, zt), (yt_hbm, yt), (xt_hbm, xt), (weight_hbm, weight), (xit_hbm, xit), (yit_hbm, yit),
             (zit_hbm, zit), (point_hbm, point), (bias_hbm, bias))
        )
    ]
    loads[0].start()
    for step in range(8):
        load_field(step).start()
    for load in loads[1:]:
        load.start()

    barrier = pltpu.get_barrier_semaphore()
    for d in range(1, 8):
        pl.semaphore_signal(barrier, inc=1, device_id={"py": wrap(py + d, 8)}, device_id_type=MESH)
    for d in range(1, 16):
        pl.semaphore_signal(barrier, inc=1, device_id={"px": wrap(px + d, 16)}, device_id_type=MESH)

    def remote(src, dst, send, recv, axis, peer):
        return pltpu.make_async_remote_copy(
            src_ref=src, dst_ref=dst, send_sem=send, recv_sem=recv, device_id={axis: peer}, device_id_type=MESH
        )

    def wait(view, semaphore):
        pltpu.make_async_copy(view, view, semaphore).wait()

    def send1(step, d, slot):
        part = pl.ds(step * 4, 4)
        peer = wrap(py + d, 8)
        return remote(z_out.at[peer, part], y_in.at[slot, part], s1, r1.at[step], "py", peer)

    def do_z(step):
        load_field(step).wait()
        z_group(field, zt, z_out, step)
        y_in[py, pl.ds(step * 4, 4)] = z_out[py, pl.ds(step * 4, 4)]

    def send_z(step):
        for d in range(1, 8):
            send1(step, d, py).start()

    loads[0].wait()
    do_z(0)
    pl.semaphore_wait(barrier, 22)
    send_z(0)

    def z_step(step, carry):
        do_z(step)
        send_z(step)
        return carry

    lax.fori_loop(1, 8, z_step, 0)

    def send2(step, peer, slot):
        return remote(y_out.at[step, peer], x_in.at[step, slot], s2, r2.at[step], "px", peer)

    def do_y(step):
        wait(y_in.at[pl.ds(0, 7), pl.ds(step * 4, 4)], r1.at[step])
        y_group(y_in, yt, y_out, y_rows, step)
        for d in range(1, 16):
            send2(step, wrap(px + d, 16), px).start()
        x_in[step, px] = y_out[step, px]

    halves = (pl.ds(0, 32), pl.ds(32, 32))

    def gather(step, phase, h, d):
        along_col = (h == 0) == (phase == 0)
        if phase == 0:
            place = spec.at[step, row, col, halves[h]]
        elif along_col:
            place = spec.at[step, :, col, halves[h]]
        else:
            place = spec.at[step, row, :, halves[h]]
        peer = 4 * row + wrap(col + d, 4) if along_col else 4 * wrap(row + d, 4) + col
        return remote(place, place, s3, r3.at[step, phase], "px", peer)

    def do_x(step):
        wait(x_in.at[step, pl.ds(0, 15)], r2.at[step])
        x_group(x_in, xt, spec, step, row, col)
        for d in (1, 3, 2):
            for h in range(2):
                gather(step, 0, h, d).start()

    def do_second(step):
        wait(spec.at[step, 0, pl.ds(0, 3)], r3.at[step, 0])
        for h in range(2):
            for d in (1, 3, 2):
                gather(step, 1, h, d).start()

    def do_mix(step):
        wait(spec.at[step, pl.ds(0, 3)], r3.at[step, 1])
        mix_group(spec, weight, sums, step)

    loads[1].wait()
    loads[2].wait()
    loads[3].wait()
    sums[...] = jnp.zeros_like(sums)
    loads[7].wait()
    spread_point(point, spread)

    def y_step(step, carry):
        do_y(step)
        point_plane(field, spread, planes, 2 * step)
        point_plane(field, spread, planes, 2 * step + 1)
        pl.when(step >= 1)(lambda: do_x(step - 1))
        pl.when(step >= 2)(lambda: do_second(step - 2))
        pl.when(step >= 5)(lambda: do_mix(step - 5))
        return carry

    lax.fori_loop(0, 8, y_step, 0)
    do_mix(3)
    do_x(7)
    do_second(6)
    do_mix(4)
    do_mix(5)
    do_second(7)
    do_mix(6)
    do_mix(7)

    loads[4].wait()
    x_inverse(sums, xit, m_out, m_rows)

    def send4(peer, slot, d):
        return remote(m_out.at[peer], b_in.at[slot], s4, r4.at[d], "px", peer)

    rows_order = (0, 1, 3, 2)
    for dr in rows_order:
        for dc in range(4):
            if dr or dc:
                peer = 4 * wrap(row - dr, 4) + wrap(col - dc, 4)
                send4(peer, px, dr).start()
    b_in[px] = m_out[px]

    last = 2
    late = pl.ds(8 * wrap(row + last, 4), 8)
    stage[2] = planes[late].astype(BF16)
    spare = pltpu.make_async_copy(stage.at[2], plane_hbm, own_sem.at[0])
    spare.start()

    def send5(dr, d):
        part = pl.ds(4 * wrap(row + dr, 4), 4)
        peer = wrap(py + d, 8)
        place = late_hbm.at[py] if dr == last else f_in.at[py, part]
        return remote(b_out.at[peer, part], place, s5, r5.at[dr], "py", peer)

    loads[5].wait()
    for dr in rows_order:
        wait(b_in.at[pl.ds(0, 4 if dr else 3)], r4.at[dr])
        part = pl.ds(4 * wrap(row + dr, 4), 4)
        y_inverse(b_in, yit, b_out, wrap(row + dr, 4))
        for d in range(1, 8):
            send5(dr, d).start()
        if dr == last:
            own = pltpu.make_async_copy(b_out.at[py, part], late_hbm.at[py], own_sem.at[1])
            own.start()
        else:
            f_in[py, part] = b_out[py, part]

    loads[6].wait()
    loads[8].wait()
    stores = []
    for n, dr in enumerate(rows_order[:3]):
        group = wrap(row + dr, 4)
        if n == 2:
            spare.wait()
        wait(f_in.at[pl.ds(0, 7), pl.ds(0, 4)], r5.at[dr])

        def final(pair, carry, n=n, group=group):
            op = 4 * group + pair
            for quad in range(4):
                g = f_in[:, op, :, :, quad * 128 : (quad + 1) * 128].reshape(128, 128)
                part = slice(4 * quad, 4 * quad + 4)
                done = activate(
                    g, [planes[2 * op + o, part] for o in range(2)], [bias[2 * op + o] for o in range(2)], zit
                )
                for o in range(2):
                    stage[n, 2 * pair + o, part] = done[o]
            return carry

        lax.fori_loop(0, 4, final, 0, unroll=2)
        store = pltpu.make_async_copy(stage.at[n], out_hbm.at[pl.ds(8 * group, 8)], out_sem.at[n])
        store.start()
        stores.append(store)
    wait(late_hbm.at[pl.ds(0, 7)], r5.at[last])
    own.wait()
    for store in stores:
        store.wait()

    wait(z_out.at[pl.ds(0, 7)], s1)
    wait(y_out.at[:, pl.ds(0, 15)], s2)
    wait(spec.at[:, 0, pl.ds(0, 3)], s3)
    wait(spec.at[:, pl.ds(0, 3)], s3)
    wait(m_out.at[pl.ds(0, 15)], s4)
    wait(b_out.at[pl.ds(0, 7)], s5)


def finish(early_hbm, late_hbm, plane_hbm, bias, zit_hbm, out_hbm, late, planes, zit, stage, held, sems):
    row = lax.axis_index("px") // 4
    group = lax.rem(row + 2, 4)

    def load_plane(quad):
        part = pl.ds(4 * quad, 4)
        return pltpu.make_async_copy(plane_hbm.at[:, part], planes.at[:, part], sems.at[quad])

    def store(quad):
        part = pl.ds(4 * quad, 4)
        return pltpu.make_async_copy(stage.at[:, part], out_hbm.at[pl.ds(8 * group, 8), part], sems.at[4 + quad])

    def through(n, j, inward):
        part = pl.ds(8 * lax.rem(row + (0, 1, 3)[n], 4) + 4 * j, 4)
        if inward:
            return pltpu.make_async_copy(early_hbm.at[part], held.at[n, j], sems.at[10 + 2 * n + j])
        return pltpu.make_async_copy(held.at[n, j], out_hbm.at[part], sems.at[16 + 2 * n + j])

    chunks = [(n, j) for n in range(3) for j in range(2)]
    first = [
        pltpu.make_async_copy(zit_hbm, zit, sems.at[8]),
        pltpu.make_async_copy(late_hbm, late, sems.at[9]),
    ]
    for copy in first:
        copy.start()
    for quad in range(4):
        load_plane(quad).start()
        if quad == 0:
            for n, j in chunks:
                through(n, j, True).start()
    for copy in first:
        copy.wait()
    for quad in range(4):
        load_plane(quad).wait()
        part = slice(4 * quad, 4 * quad + 4)
        for pair in range(4):
            g = late[:, pair, :, :, quad * 128 : (quad + 1) * 128].reshape(128, 128)
            done = activate(
                g,
                [planes[2 * pair + o, part].astype(F32) for o in range(2)],
                [bias[8 * group + 2 * pair + o] for o in range(2)],
                zit,
            )
            for o in range(2):
                stage[2 * pair + o, part] = done[o]
        store(quad).start()
        for n, j in chunks[2 * quad : 2 * quad + 2]:
            through(n, j, True).wait()
            through(n, j, False).start()
    for quad in range(4):
        store(quad).wait()
    for n, j in chunks:
        through(n, j, False).wait()


def body(tables, field, spectral_weight, point_weight, point_bias):
    z_table, y_table, x_table, xi_table, yi_table, zi_table = tables
    field = field.reshape(32, 16, 32, 256)
    anywhere = pl.BlockSpec(memory_space=pl.ANY)
    dma = pltpu.SemaphoreType.DMA
    operands = (field, spectral_weight, z_table, y_table, x_table, xi_table, yi_table, zi_table, point_weight)
    early, late, planes = pl.pallas_call(
        transform,
        out_shape=(
            jax.ShapeDtypeStruct((32, 16, 32, 256), BF16),
            jax.ShapeDtypeStruct((8, 4, 2, 8, 512), BF16),
            jax.ShapeDtypeStruct((8, 16, 32, 256), BF16),
        ),
        in_specs=[anywhere] * (len(operands) + 1),
        out_specs=(anywhere,) * 3,
        scratch_shapes=[
            *[pltpu.VMEM(a.shape, a.dtype) for a in operands],
            pltpu.SMEM((32,), F32),
            pltpu.VMEM((8, 32, 8, 512), BF16),
            pltpu.VMEM((8, 32, 8, 512), BF16),
            pltpu.VMEM((256, 128), F32),
            pltpu.VMEM((8, 16, 16, 128), BF16),
            pltpu.VMEM((8, 16, 16, 128), BF16),
            pltpu.VMEM((8, 4, 4, 64, 128), BF16),
            pltpu.VMEM((2, 4, 2, 64, 64), F32),
            pltpu.VMEM((2048, 128), F32),
            pltpu.VMEM((16, 128, 128), BF16),
            pltpu.VMEM((16, 128, 128), BF16),
            pltpu.VMEM((8, 16, 2, 8, 512), BF16),
            pltpu.VMEM((256, 256), BF16),
            pltpu.VMEM((32, 16, 32, 256), F32),
            pltpu.VMEM((8, 16, 2, 8, 512), BF16),
            pltpu.VMEM((3, 8, 16, 32, 256), BF16),
            dma((9,)), dma((8,)),
            dma, dma((8,)),
            dma, dma((8,)),
            dma, dma((8, 2)),
            dma, dma((4,)),
            dma, dma((4,)),
            dma((2,)), dma((3,)),
        ],
        compiler_params=pltpu.CompilerParams(
            collective_id=1, has_side_effects=True, vmem_limit_bytes=VMEM_LIMIT
        ),
        name="transform",
    )(*operands, point_bias)
    out = pl.pallas_call(
        finish,
        out_shape=jax.ShapeDtypeStruct((32, 16, 32, 256), BF16),
        in_specs=[anywhere] * 3 + [pl.BlockSpec(memory_space=pltpu.SMEM), anywhere],
        out_specs=anywhere,
        scratch_shapes=[
            pltpu.VMEM((8, 4, 2, 8, 512), BF16),
            pltpu.VMEM((8, 16, 32, 256), BF16),
            pltpu.VMEM((256, 512), BF16),
            pltpu.VMEM((8, 16, 32, 256), BF16),
            pltpu.VMEM((3, 2, 4, 16, 32, 256), BF16),
            dma((22,)),
        ],
        compiler_params=pltpu.CompilerParams(vmem_limit_bytes=VMEM_LIMIT),
        name="finish",
    )(early, late, planes, point_bias, zi_table)
    return out.reshape(1, 32, 16, 32, 256)


def solution(mesh):
    tables = tuple(jnp.asarray(t) for t in build_tables())

    def run(field, spectral_weight, point_weight, point_bias):
        return jax.shard_map(
            body,
            mesh=mesh,
            in_specs=((P(),) * 6, P(None, None, "px", "py", None), P(None, None, "px", "py", None, None), P(), P()),
            out_specs=P(None, None, "px", "py", None),
            check_vma=False,
        )(tables, field, spectral_weight, point_weight, point_bias)

    return run
```
